32 devices in a mesh: expert: 16 (over z, y, x), dp: 2 (over core).
Axes of the slice: x: 2, y: 2, z: 4, core: 2. Of those that a mesh axis runs over, the one named last changes fastest.
Arguments:
- tokens: bfloat16 [1024, 3584], P(('dp', 'expert')), parts along dimension 0, may hold values from -6 to 6
- expert_ids: int32 [1024, 8], P(('dp', 'expert')), parts along dimension 0, may hold values from 0 to 11, as said below
- gate_weights: float32 [1024, 8], P(('dp', 'expert')), parts along dimension 0, may hold values from 0.05 to 0.5
- placement_table: int32 [24, 2], P('dp'), parts along dimension 0, may hold values from 0 to 15, as said below
- replica_choice: int32 [1024, 8], P(('dp', 'expert')), parts along dimension 0, may hold values from 0 to 1
- w_gate: bfloat16 [16, 3584, 1024], P('expert'), may hold values from -0.09375 to 0.09375
- w_up: bfloat16 [16, 3584, 1024], P('expert'), may hold values from -0.09375 to 0.09375
- w_down: bfloat16 [16, 1024, 3584], P('expert'), may hold values from -0.1875 to 0.1875
Outputs:
- mixed: bfloat16 [1024, 3584], P(('dp', 'expert')), parts along dimension 0
- slot_load: float32 [32], P(('dp', 'expert')), parts along dimension 0
The draws below stay inside these ranges and needn't reach their ends.
There are 2 independent parts, one for each index of `dp`. The reference program is written for one: setup_inputs(seed, part) draws one part's arguments, and reference() takes and returns one part's arrays. A program takes and returns all parts, laid end to end along the dimension named above; an argument that names none is the same for every part. Nothing has to cross between parts.
Inputs may be any that keep to these rules, and one draw needn't show every extreme that they name: `expert_ids`: each row names 8 different logical experts, hot experts chosen more often. `placement_table`: every slot of 0 to 15 appears for exactly one expert; 4 experts have two different slots, every other expert has the same slot in both columns. `replica_choice`: a column of the placement table.
All inputs are finite; a program needn't handle non-finite values.
Results may differ from the reference program's by a relative error of at most 0.0025.
Values may be sent and summed in bfloat16 or wider, within the bound.
A program may use at most 128 MiB of HBM per device.

```python
import math
import jax
import jax.numpy as jnp
from jax import lax

D = 3584
FF = 1024
TOP = 8
TOK_DEV = 32
SLOTS = 16
EXPERTS = 12
TOKENS = 512
CAP = 21
N_EXPERT = 16


def layout_plan(key):
    popular_expert_total = SLOTS - EXPERTS
    order = jax.random.permutation(jax.random.fold_in(key, 11), EXPERTS)
    hot_list = order[:popular_expert_total].astype(jnp.int32)
    flag_popular = jnp.zeros((EXPERTS,), jnp.int32).at[hot_list].set(1)
    popular_position = jnp.zeros((EXPERTS,), jnp.int32).at[hot_list].set(jnp.arange(popular_expert_total, dtype=jnp.int32))
    slot_order = jax.random.permutation(jax.random.fold_in(key, 12), SLOTS).astype(jnp.int32)
    first_slot = slot_order[:EXPERTS]
    second_pool = slot_order[EXPERTS:]
    second_slot = jnp.where(flag_popular == 1, second_pool[popular_position], first_slot)
    table = jnp.stack([first_slot, second_slot], axis=1).astype(jnp.int32)
    return (table, flag_popular, popular_position)


def draw_placement_table(key, part):
    table, flag_popular, popular_position = layout_plan(key)
    return table


def draw_expert_ids(key, part):
    table, flag_popular, popular_position = layout_plan(key)
    popular_expert_total = SLOTS - EXPERTS
    extra_reward = flag_popular * ((popular_expert_total - popular_position) * 4096 // popular_expert_total)
    routing_logits = jax.random.randint(jax.random.fold_in(key, 13), (TOKENS, EXPERTS), 0, 65536, dtype=jnp.int32)
    routing_logits = routing_logits + extra_reward[None, :]
    distinct = routing_logits * EXPERTS + jnp.arange(EXPERTS, dtype=jnp.int32)[None, :]
    chosen = jax.lax.top_k(distinct, TOP)[1]
    return chosen.astype(jnp.int32)


def plant(array, stream_key, low, largest):
    spot = [jax.random.randint(jax.random.fold_in(stream_key, axis), (), 0, length) for axis, length in enumerate(array.shape)]
    longest = array.shape.index(max(array.shape))
    neighbour = spot[:longest] + [(spot[longest] + 1) % array.shape[longest]] + spot[longest + 1:]
    return array.at[tuple(spot)].set(low).at[tuple(neighbour)].set(largest)


def block_levels(own_key, extent, shards, least, high):
    factor_of, own = 1.0, jax.random.fold_in(own_key, 6)
    for dim, shards_of in shards:
        steps = jnp.exp(jax.random.uniform(jax.random.fold_in(own, dim), (shards_of,), jnp.float32, least / len(shards), high / len(shards)))
        factor_of = factor_of * jnp.repeat(steps, extent[dim] // shards_of).reshape([-1 if axis == dim else 1 for axis in range(len(extent))])
    return factor_of


def centred(stream_key, dims, deviation, bound, shards=(), kind=jnp.bfloat16):
    array = deviation * jax.random.normal(stream_key, dims, jnp.float32)
    if shards:
        array = array * block_levels(stream_key, dims, shards, -0.22, 0.18)
    return jnp.clip(array, -bound, bound).astype(kind)


def setup_inputs(seed: int = 0, part: int = 0) -> dict:
    seeds = jax.random.split(jax.random.key(seed), 9)
    part_splits = jax.random.split(jax.random.fold_in(seeds[8], part), 9)
    return {
        "tokens": centred(part_splits[0], (TOKENS, D), 1.0, 6.0, ((0, 16),)),
        "expert_ids": draw_expert_ids(jax.random.fold_in(jax.random.fold_in(seeds[8], part), 71), part),
        "gate_weights": jnp.clip(jnp.exp(math.log(0.5) - 2.3025851 * jax.random.uniform(part_splits[2], (TOKENS, TOP), jnp.float32) ** block_levels(part_splits[2], (TOKENS, TOP), ((0, 16),), -0.2, 0.2)), 0.05, 0.5),
        "placement_table": draw_placement_table(jax.random.fold_in(jax.random.fold_in(seeds[8], part), 71), part),
        "replica_choice": plant(jax.random.randint(part_splits[4], (TOKENS, TOP), 0, 2), jax.random.fold_in(part_splits[4], 1), 0, 1).astype(jnp.int32),
        "w_gate": centred(seeds[5], (SLOTS, D, FF), D ** -0.5, 0.09375, ((0, 16),)),
        "w_up": centred(seeds[6], (SLOTS, D, FF), D ** -0.5, 0.09375, ((0, 16),)),
        "w_down": centred(seeds[7], (SLOTS, FF, D), FF ** -0.5, 0.1875, ((0, 16),)),
    }


def group_positions(row_slots):
    onehot = (row_slots[:, None] == jnp.arange(SLOTS, dtype=jnp.int32)[None, :]).astype(jnp.int32)
    running = jnp.cumsum(onehot, axis=0)
    return jnp.take_along_axis(running, row_slots[:, None], axis=1)[:, 0] - 1


def reference(tokens, expert_ids, gate_weights, placement_table, replica_choice, w_gate, w_up, w_down):
    slot_ids = placement_table[expert_ids, replica_choice].astype(jnp.int32)
    grouped = slot_ids.reshape(N_EXPERT, TOK_DEV * TOP)
    position = lax.map(group_positions, grouped).reshape(TOKENS, TOP)
    retained_selector = position < CAP
    source = (jnp.arange(TOKENS, dtype=jnp.int32) // TOK_DEV)[:, None]
    table_rows = SLOTS * N_EXPERT * CAP
    flat = jnp.where(retained_selector, (slot_ids * N_EXPERT + source) * CAP + position, table_rows).reshape(-1)
    token_index = jnp.arange(TOKENS * TOP, dtype=jnp.int32) // TOP
    source_item_index = jnp.full((table_rows,), TOKENS, jnp.int32).at[flat].set(token_index, mode="drop")
    gate_of = jnp.zeros((table_rows,), jnp.float32).at[flat].set(gate_weights.reshape(-1), mode="drop")
    source_item_index = source_item_index.reshape(SLOTS, N_EXPERT * CAP)
    gate_of = gate_of.reshape(SLOTS, N_EXPERT * CAP)
    padded = jnp.concatenate([tokens, jnp.zeros((1, D), tokens.dtype)], axis=0)

    def one_slot(carry, inputs):
        row_index, gates, gate_w, up_w, down_w = inputs
        rows = padded[row_index]
        gate_part = jnp.dot(rows, gate_w, preferred_element_type=jnp.float32)
        up_part = jnp.dot(rows, up_w, preferred_element_type=jnp.float32)
        hidden = (jax.nn.silu(gate_part) * up_part).astype(jnp.bfloat16)
        output = jnp.dot(hidden, down_w, preferred_element_type=jnp.float32).astype(jnp.bfloat16)
        carry = carry.at[row_index].add(gates[:, None] * output.astype(jnp.float32), mode="drop")
        return carry, None

    start = jnp.zeros((TOKENS, D), jnp.float32)
    mixed, _ = lax.scan(one_slot, start, (source_item_index, gate_of, w_gate, w_up, w_down))
    counts = jnp.zeros((SLOTS,), jnp.float32).at[slot_ids.reshape(-1)].add(retained_selector.reshape(-1).astype(jnp.float32))
    slot_load = counts * (SLOTS / (TOKENS * TOP))
    return mixed.astype(jnp.bfloat16), slot_load
```

```python
import functools

import jax
import jax.numpy as jnp
from jax import lax
from jax.experimental import pallas as pl
from jax.experimental.pallas import tpu as pltpu
from jax.sharding import PartitionSpec as P

PLANE = 4
LANES = 128
VMEM_BYTES = 64 * 1000 * 1000


def run_experts(received, gate_w, up_w, down_w):
    peers, capacity, hidden_dimension = received.shape
    rows = received.reshape(peers * capacity, hidden_dimension)
    gate_part = jnp.dot(rows, gate_w, preferred_element_type=jnp.float32)
    up_part = jnp.dot(rows, up_w, preferred_element_type=jnp.float32)
    hidden = (jax.nn.silu(gate_part) * up_part).astype(jnp.bfloat16)
    output = jnp.dot(hidden, down_w, preferred_element_type=jnp.float32).astype(jnp.bfloat16)
    return output.reshape(peers, capacity, hidden_dimension)


def per_device_exchange(
    tokens, expert_ids, gate_weights, placement_table, replica_choice, w_gate, w_up, w_down
):
    devices = lax.axis_size("expert")
    tok_rows, top_count = expert_ids.shape
    hidden_dimension = tokens.shape[1]
    slot_total = devices
    capacity = 5 * tok_rows * top_count // (4 * slot_total) + 1
    slot_ids = placement_table[expert_ids, replica_choice].astype(jnp.int32).reshape(-1)
    onehot = (slot_ids[:, None] == jnp.arange(slot_total, dtype=jnp.int32)[None, :]).astype(
        jnp.int32
    )
    running = jnp.cumsum(onehot, axis=0)
    position = jnp.sum(running * onehot, axis=1) - 1
    retained_selector = position < capacity
    table_rows = slot_total * capacity
    flat = jnp.where(retained_selector, slot_ids * capacity + position, table_rows)
    token_index = jnp.arange(tok_rows * top_count, dtype=jnp.int32) // top_count
    source_item_index = (
        jnp.full((table_rows,), tok_rows, jnp.int32).at[flat].set(token_index, mode="drop")
    )
    padded = jnp.concatenate([tokens, jnp.zeros((1, hidden_dimension), tokens.dtype)], axis=0)
    outgoing = padded[source_item_index].reshape(devices, capacity, hidden_dimension)
    incoming = lax.all_to_all(outgoing, "expert", split_axis=0, concat_axis=0, tiled=True)
    results = run_experts(incoming, w_gate[0], w_up[0], w_down[0])
    returned = lax.all_to_all(results, "expert", split_axis=0, concat_axis=0, tiled=True)
    returned = returned.reshape(table_rows, hidden_dimension)
    pair_rows = returned[jnp.minimum(flat, table_rows - 1)].reshape(
        tok_rows, top_count, hidden_dimension
    )
    weights = jnp.where(retained_selector.reshape(tok_rows, top_count), gate_weights, 0.0).astype(
        jnp.float32
    )
    mixed = jnp.sum(weights[:, :, None] * pair_rows.astype(jnp.float32), axis=1).astype(
        jnp.bfloat16
    )
    counts = jnp.sum(onehot * retained_selector.astype(jnp.int32)[:, None], axis=0).astype(
        jnp.float32
    )
    own_counts = lax.psum_scatter(counts, "expert", scatter_dimension=0, tiled=True)
    slot_load = own_counts * (slot_total / (tok_rows * devices * top_count))
    return (mixed, slot_load)


def tile_of(size, wanted):
    tile = min(size, wanted)
    while size % tile:
        tile -= LANES
    return tile


def kernel(
    n, rows, top, cap, depth, hidden,
    ext_ref, gates_ref, wg_hbm, wu_hbm, wd_hbm,
    mixed_ref, load_ref,
    gathered, wg, wu, wd, packed, mid, outgoing, incoming, acc,
    w_sem, own_sem, ag_send, ag_recv, ret_send, ret_recv, local_sem,
):
    planes = n // PLANE
    pad = outgoing.shape[1] * outgoing.shape[2]
    me = lax.axis_index("expert")
    z = me // PLANE
    q = me % PLANE
    y, x = q // 2, q % 2
    x_peer = y * 2 + (1 - x)
    y_peer = (1 - y) * 2 + x
    d_peer = (1 - y) * 2 + (1 - x)
    half = rows // 2

    weight_copies = [
        pltpu.make_async_copy(src.at[0], dst, w_sem.at[i])
        for i, (src, dst) in enumerate(((wg_hbm, wg), (wu_hbm, wu), (wd_hbm, wd)))
    ]
    own = pltpu.make_async_copy(ext_ref, gathered.at[me], own_sem)
    own.start()
    for copy in weight_copies:
        copy.start()

    barrier = pltpu.get_barrier_semaphore()
    for other in range(1, n):
        pl.semaphore_signal(
            barrier, inc=1, device_id={"expert": lax.rem(me + other, n)},
            device_id_type=pl.DeviceIdType.MESH,
        )
    pl.semaphore_wait(barrier, n - 1)
    own.wait()

    def send(group, plane, kind_send, kind_recv, target, first=0, count=None):
        count = rows if count is None else count
        part = gathered.at[group, pl.ds(first, count)]
        return pltpu.make_async_remote_copy(
            src_ref=part, dst_ref=part,
            send_sem=ag_send.at[plane, kind_send], recv_sem=ag_recv.at[plane, kind_recv],
            device_id={"expert": target}, device_id_type=pl.DeviceIdType.MESH,
        )

    def plane_at(b):
        low = jnp.minimum(z, planes - 1 - z)
        near = low + ((b + 1) // 2) * (1 if b % 2 else -1)
        pick = jnp.where(b <= 2 * low, near, b)
        return jnp.where(z < planes - z, pick, planes - 1 - pick) if planes > 1 else z

    order = [plane_at(b) for b in range(planes)]

    def up_of(p):
        return send(p * PLANE + q, p, 0, 0, me + PLANE)

    def down_of(p):
        return send(p * PLANE + q, p, 1, 0, me - PLANE)

    def to_x(p):
        return send(p * PLANE + q, p, 2, 1, z * PLANE + x_peer)

    def to_y(p):
        return send(p * PLANE + q, p, 3, 2, z * PLANE + y_peer)

    def relay_y(p):
        return send(p * PLANE + x_peer, p, 4, 3, z * PLANE + y_peer, 0, half)

    def relay_x(p):
        return send(p * PLANE + y_peer, p, 5, 4, z * PLANE + x_peer, half, half)

    def wait_in(p, position, kind, first=0, count=None):
        count = rows if count is None else count
        part = gathered.at[p * PLANE + position, pl.ds(first, count)]
        pltpu.make_async_copy(part, part, ag_recv.at[p, kind]).wait()

    def column_stage(p):
        @pl.when(p != z)
        def _():
            wait_in(p, q, 0)

        @pl.when((p <= z) & (z < planes - 1))
        def _():
            up_of(p).start()

        @pl.when((p >= z) & (z > 0))
        def _():
            down_of(p).start()

        to_x(p).start()
        to_y(p).start()

    def relay_stage(p):
        wait_in(p, x_peer, 1)
        relay_y(p).start()
        wait_in(p, y_peer, 2)
        relay_x(p).start()

    def diagonal_stage(p):
        wait_in(p, d_peer, 3, 0, half)
        wait_in(p, d_peer, 4, half, half)

    def return_copy(group):
        return pltpu.make_async_remote_copy(
            src_ref=outgoing.at[group], dst_ref=incoming.at[me],
            send_sem=ret_send.at[group], recv_sem=ret_recv.at[me],
            device_id={"expert": group}, device_id_type=pl.DeviceIdType.MESH,
        )

    def own_return():
        return pltpu.make_async_copy(outgoing.at[me], incoming.at[me], local_sem)

    batch_tokens = PLANE * rows
    batch_rows = PLANE * pad
    t_i = lax.broadcasted_iota(jnp.int32, (batch_tokens, batch_tokens), 0)
    t_j = lax.broadcasted_iota(jnp.int32, (batch_tokens, batch_tokens), 1)
    before = ((t_j < t_i) & (t_j // rows == t_i // rows)).astype(jnp.bfloat16)
    lane = lax.broadcasted_iota(jnp.int32, (batch_tokens, batch_rows), 1).astype(jnp.float32)
    base = (
        lax.broadcasted_iota(jnp.int32, (batch_tokens, batch_rows), 0) // rows * pad
    ).astype(jnp.float32)
    me_f = me.astype(jnp.float32)
    ff_tile = tile_of(hidden, 256)
    d_tile = tile_of(depth, 512)

    def compute(p, first):
        ids = gathered[pl.ds(p * PLANE, PLANE), :, depth:].reshape(batch_tokens, LANES)
        hit = jnp.sum((ids.astype(jnp.float32) == me_f).astype(jnp.float32), axis=1, keepdims=True)
        pos = jnp.dot(
            before, jnp.broadcast_to(hit, (batch_tokens, batch_rows)).astype(jnp.bfloat16),
            preferred_element_type=jnp.float32,
        )
        kept = (hit > 0.5) & (pos < cap - 0.5)
        chosen = (kept & (lane == base + pos)).astype(jnp.float32)
        load_ref[...] += jnp.sum(chosen)
        chosen = chosen.astype(jnp.bfloat16)

        @pl.loop(0, depth // d_tile)
        def _(i):
            cols = pl.ds(pl.multiple_of(i * d_tile, d_tile), d_tile)
            block = gathered[pl.ds(p * PLANE, PLANE), :, cols].reshape(batch_tokens, d_tile)
            packed[:, cols] = lax.dot_general(
                chosen, block, (((0,), (0,)), ((), ())), preferred_element_type=jnp.float32
            ).astype(jnp.bfloat16)

        if first:
            weight_copies[0].wait()
            weight_copies[1].wait()

        @pl.loop(0, hidden // ff_tile)
        def _(i):
            cols = pl.ds(pl.multiple_of(i * ff_tile, ff_tile), ff_tile)
            gate = jnp.dot(packed[...], wg[:, cols], preferred_element_type=jnp.float32)
            up = jnp.dot(packed[...], wu[:, cols], preferred_element_type=jnp.float32)
            mid[:, cols] = (gate / (1.0 + jnp.exp(-gate)) * up).astype(jnp.bfloat16)

        if first:
            weight_copies[2].wait()

        @pl.loop(0, depth // d_tile)
        def _(i):
            cols = pl.ds(pl.multiple_of(i * d_tile, d_tile), d_tile)
            out = jnp.dot(mid[...], wd[:, cols], preferred_element_type=jnp.float32)
            outgoing[pl.ds(p * PLANE, PLANE), :, :, cols] = out.reshape(
                PLANE, outgoing.shape[1], outgoing.shape[2], d_tile
            ).astype(jnp.bfloat16)

        for j in range(PLANE):
            group = p * PLANE + j

            @pl.when(group != me)
            def _():
                return_copy(group).start()

            @pl.when(group == me)
            def _():
                own_return().start()

    load_ref[...] = jnp.zeros_like(load_ref)
    column_stage(order[0])
    relay_stage(order[0])
    for b in range(planes):
        if b + 1 < planes:
            column_stage(order[b + 1])
        diagonal_stage(order[b])
        compute(order[b], b == 0)
        if b + 1 < planes:
            relay_stage(order[b + 1])
    load_ref[...] = load_ref[...] * (n / (rows * n * top))

    ids = gathered[me, :, depth:].astype(jnp.float32)
    own_lane = lax.broadcasted_iota(jnp.int32, (rows, LANES), 1).astype(jnp.float32)
    slots = [ids[:, k : k + 1] for k in range(top)]
    hits = functools.reduce(jnp.add, [(s == own_lane).astype(jnp.float32) for s in slots])
    r_i = lax.broadcasted_iota(jnp.int32, (rows, rows), 0)
    r_j = lax.broadcasted_iota(jnp.int32, (rows, rows), 1)
    positions = jnp.dot(
        (r_j < r_i).astype(jnp.bfloat16), hits.astype(jnp.bfloat16),
        preferred_element_type=jnp.float32,
    )
    columns, weights = [], []
    for k in range(top):
        at = jnp.sum(jnp.where(slots[k] == own_lane, positions, 0.0), axis=1, keepdims=True)
        columns.append(slots[k] * pad + at)
        weights.append(jnp.where(at < cap - 0.5, gates_ref[:, k : k + 1], 0.0))
    col_lane = lax.broadcasted_iota(jnp.int32, (rows, batch_rows), 1).astype(jnp.float32)

    for b in range(planes):
        p = order[b]
        for j in range(PLANE):
            source = p * PLANE + j

            @pl.when(source != me)
            def _():
                block = incoming.at[source]
                pltpu.make_async_copy(block, block, ret_recv.at[source]).wait()

            @pl.when(source == me)
            def _():
                own_return().wait()

        shift = (p * batch_rows).astype(jnp.float32)
        share = functools.reduce(
            jnp.add,
            [jnp.where(c - shift == col_lane, w, 0.0) for c, w in zip(columns, weights)],
        )
        high = share.astype(jnp.bfloat16)
        rest = share - high.astype(jnp.float32)
        middle = rest.astype(jnp.bfloat16)
        low = (rest - middle.astype(jnp.float32)).astype(jnp.bfloat16)
        spread = jnp.concatenate([high, middle, low], axis=0)

        @pl.loop(0, depth // d_tile)
        def _(i):
            cols = pl.ds(pl.multiple_of(i * d_tile, d_tile), d_tile)
            block = incoming[pl.ds(p * PLANE, PLANE), :, :, cols].astype(jnp.float32)
            block = block.reshape(batch_rows, d_tile).astype(jnp.bfloat16)
            sums = jnp.dot(spread, block, preferred_element_type=jnp.float32)
            sums = sums[:rows] + (sums[rows : 2 * rows] + sums[2 * rows :])
            if b > 0:
                sums = acc[:, cols] + sums
            if b < planes - 1:
                acc[:, cols] = sums
            else:
                mixed_ref[:, cols] = sums.astype(jnp.bfloat16)

    for b in range(planes):
        p = order[b]

        @pl.when((p <= z) & (z < planes - 1))
        def _():
            up_of(p).wait_send()

        @pl.when((p >= z) & (z > 0))
        def _():
            down_of(p).wait_send()

        to_x(p).wait_send()
        to_y(p).wait_send()
        relay_y(p).wait_send()
        relay_x(p).wait_send()
        for j in range(PLANE):
            group = p * PLANE + j

            @pl.when(group != me)
            def _():
                return_copy(group).wait_send()


def per_device_gathered(
    tokens, expert_ids, gate_weights, placement_table, replica_choice, w_gate, w_up, w_down
):
    n = lax.axis_size("expert")
    rows, top = expert_ids.shape
    depth = tokens.shape[1]
    hidden = w_gate.shape[2]
    cap = 5 * rows * top // (4 * n) + 1
    slabs = -(-cap // 8)
    experts = placement_table.shape[0]
    pick = expert_ids[:, :, None] == jnp.arange(experts, dtype=jnp.int32)
    both = jnp.where(
        replica_choice[:, :, None] == 0, placement_table[:, 0], placement_table[:, 1]
    )
    slot_ids = jnp.sum(jnp.where(pick, both, 0), axis=2)
    slot_cols = jnp.pad(
        slot_ids.astype(tokens.dtype), ((0, 0), (0, LANES - top)), constant_values=-1
    )
    ext = jnp.concatenate([tokens, slot_cols], axis=1)
    planes = n // PLANE
    bf16, f32 = jnp.bfloat16, jnp.float32
    anywhere = pl.BlockSpec(memory_space=pl.ANY)
    vmem = pl.BlockSpec(memory_space=pltpu.VMEM)
    mixed, load = pl.pallas_call(
        functools.partial(kernel, n, rows, top, cap, depth, hidden),
        out_shape=(
            jax.ShapeDtypeStruct((rows, depth), bf16),
            jax.ShapeDtypeStruct((8, LANES), f32),
        ),
        in_specs=[anywhere, vmem, anywhere, anywhere, anywhere],
        out_specs=(vmem, vmem),
        scratch_shapes=[
            pltpu.VMEM((n, rows, depth + LANES), bf16),
            pltpu.VMEM((depth, hidden), bf16),
            pltpu.VMEM((depth, hidden), bf16),
            pltpu.VMEM((hidden, depth), bf16),
            pltpu.VMEM((PLANE * slabs * 8, depth), bf16),
            pltpu.VMEM((PLANE * slabs * 8, hidden), bf16),
            pltpu.VMEM((n, slabs, 8, depth), bf16),
            pltpu.VMEM((n, slabs, 8, depth), bf16),
            pltpu.VMEM((rows, depth), f32),
            pltpu.SemaphoreType.DMA((3,)),
            pltpu.SemaphoreType.DMA,
            pltpu.SemaphoreType.DMA((planes, 6)),
            pltpu.SemaphoreType.DMA((planes, 5)),
            pltpu.SemaphoreType.DMA((n,)),
            pltpu.SemaphoreType.DMA((n,)),
            pltpu.SemaphoreType.DMA,
        ],
        compiler_params=pltpu.CompilerParams(
            collective_id=0, has_side_effects=True, vmem_limit_bytes=VMEM_BYTES
        ),
    )(ext, gate_weights, w_gate, w_up, w_down)
    return mixed, load[0, :1]


def solution(mesh):
    placed = (
        P(("dp", "expert"), None),
        P(("dp", "expert"), None),
        P(("dp", "expert"), None),
        P("dp", None),
        P(("dp", "expert"), None),
        P("expert", None, None),
        P("expert", None, None),
        P("expert", None, None),
    )

    def per_device(*args):
        n = mesh.shape["expert"]
        rows, depth = args[0].shape
        weights = 3 * args[5].size
        blocks = n * rows * (depth + LANES) + 2 * n * (rows + 8) * depth
        fits = 2 * (weights + blocks) < 3 * VMEM_BYTES // 4
        if fits and n % PLANE == 0 and n <= LANES and rows % 16 == 0:
            return per_device_gathered(*args)
        return per_device_exchange(*args)

    return jax.shard_map(
        per_device,
        mesh=mesh,
        in_specs=placed,
        out_specs=(P(("dp", "expert"), None), P(("dp", "expert"))),
        check_vma=False,
    )
```

```python
import functools

import jax
import jax.numpy as jnp
from jax import lax
from jax.experimental import pallas as pl
from jax.experimental.pallas import tpu as pltpu
from jax.sharding import PartitionSpec as P

PLANE = 4
LANES = 128
VMEM_BYTES = 64 * 1000 * 1000


def run_experts(received, gate_w, up_w, down_w):
    peers, capacity, hidden_dimension = received.shape
    rows = received.reshape(peers * capacity, hidden_dimension)
    gate_part = jnp.dot(rows, gate_w, preferred_element_type=jnp.float32)
    up_part = jnp.dot(rows, up_w, preferred_element_type=jnp.float32)
    hidden = (jax.nn.silu(gate_part) * up_part).astype(jnp.bfloat16)
    output = jnp.dot(hidden, down_w, preferred_element_type=jnp.float32).astype(jnp.bfloat16)
    return output.reshape(peers, capacity, hidden_dimension)


def per_device_exchange(
    tokens, expert_ids, gate_weights, placement_table, replica_choice, w_gate, w_up, w_down
):
    devices = lax.axis_size("expert")
    tok_rows, top_count = expert_ids.shape
    hidden_dimension = tokens.shape[1]
    slot_total = devices
    capacity = 5 * tok_rows * top_count // (4 * slot_total) + 1
    slot_ids = placement_table[expert_ids, replica_choice].astype(jnp.int32).reshape(-1)
    onehot = (slot_ids[:, None] == jnp.arange(slot_total, dtype=jnp.int32)[None, :]).astype(
        jnp.int32
    )
    running = jnp.cumsum(onehot, axis=0)
    position = jnp.sum(running * onehot, axis=1) - 1
    retained_selector = position < capacity
    table_rows = slot_total * capacity
    flat = jnp.where(retained_selector, slot_ids * capacity + position, table_rows)
    token_index = jnp.arange(tok_rows * top_count, dtype=jnp.int32) // top_count
    source_item_index = (
        jnp.full((table_rows,), tok_rows, jnp.int32).at[flat].set(token_index, mode="drop")
    )
    padded = jnp.concatenate([tokens, jnp.zeros((1, hidden_dimension), tokens.dtype)], axis=0)
    outgoing = padded[source_item_index].reshape(devices, capacity, hidden_dimension)
    incoming = lax.all_to_all(outgoing, "expert", split_axis=0, concat_axis=0, tiled=True)
    results = run_experts(incoming, w_gate[0], w_up[0], w_down[0])
    returned = lax.all_to_all(results, "expert", split_axis=0, concat_axis=0, tiled=True)
    returned = returned.reshape(table_rows, hidden_dimension)
    pair_rows = returned[jnp.minimum(flat, table_rows - 1)].reshape(
        tok_rows, top_count, hidden_dimension
    )
    weights = jnp.where(retained_selector.reshape(tok_rows, top_count), gate_weights, 0.0).astype(
        jnp.float32
    )
    mixed = jnp.sum(weights[:, :, None] * pair_rows.astype(jnp.float32), axis=1).astype(
        jnp.bfloat16
    )
    counts = jnp.sum(onehot * retained_selector.astype(jnp.int32)[:, None], axis=0).astype(
        jnp.float32
    )
    own_counts = lax.psum_scatter(counts, "expert", scatter_dimension=0, tiled=True)
    slot_load = own_counts * (slot_total / (tok_rows * devices * top_count))
    return (mixed, slot_load)


def tile_of(size, wanted):
    tile = min(size, wanted)
    while size % tile:
        tile -= LANES
    return tile


def kernel(
    n, rows, top, cap, depth, hidden,
    table_ref, tokens_hbm, ids_ref, choice_ref, gates_ref, wg_hbm, wu_hbm, wd_hbm,
    mixed_ref, load_ref,
    gathered, wg, wu, wd, packed, mid, outgoing, incoming, acc,
    w_sem, own_sem, ag_send, ag_recv, ret_send, ret_recv, local_sem,
):
    planes = n // PLANE
    pad = outgoing.shape[1] * outgoing.shape[2]
    me = lax.axis_index("expert")
    z = me // PLANE
    q = me % PLANE
    y, x = q // 2, q % 2
    x_peer = y * 2 + (1 - x)
    y_peer = (1 - y) * 2 + x
    d_peer = (1 - y) * 2 + (1 - x)
    half = rows // 2

    weight_copies = [
        pltpu.make_async_copy(src.at[0], dst, w_sem.at[i])
        for i, (src, dst) in enumerate(((wg_hbm, wg), (wu_hbm, wu), (wd_hbm, wd)))
    ]
    own = pltpu.make_async_copy(tokens_hbm, gathered.at[me, :, pl.ds(0, depth)], own_sem)
    own.start()
    slot_rows = jnp.zeros((top, rows), jnp.int32)
    for e in range(table_ref.shape[1]):
        pair = jnp.where(choice_ref[...] == 0, table_ref[0, e], table_ref[1, e])
        slot_rows = jnp.where(ids_ref[...] == e, pair, slot_rows)
    eye = (
        lax.broadcasted_iota(jnp.int32, (top, LANES), 0)
        == lax.broadcasted_iota(jnp.int32, (top, LANES), 1)
    ).astype(jnp.bfloat16)

    def turned(block):
        return lax.dot_general(
            block, eye, (((0,), (0,)), ((), ())), preferred_element_type=jnp.float32
        )

    slot_cols = turned(slot_rows.astype(jnp.float32).astype(jnp.bfloat16))
    k_lane = lax.broadcasted_iota(jnp.int32, (rows, LANES), 1)
    gathered[me, :, depth:] = jnp.where(k_lane < top, slot_cols, -1.0).astype(jnp.bfloat16)
    for copy in weight_copies:
        copy.start()

    barrier = pltpu.get_barrier_semaphore()
    for other in range(1, n):
        pl.semaphore_signal(
            barrier, inc=1, device_id={"expert": lax.rem(me + other, n)},
            device_id_type=pl.DeviceIdType.MESH,
        )
    pl.semaphore_wait(barrier, n - 1)
    own.wait()

    def send(group, plane, kind_send, kind_recv, target, first=0, count=None):
        count = rows if count is None else count
        part = gathered.at[group, pl.ds(first, count)]
        return pltpu.make_async_remote_copy(
            src_ref=part, dst_ref=part,
            send_sem=ag_send.at[plane, kind_send], recv_sem=ag_recv.at[plane, kind_recv],
            device_id={"expert": target}, device_id_type=pl.DeviceIdType.MESH,
        )

    z_half = planes // 2
    low = jnp.minimum(z, planes - 1 - z)

    def plane_at(b):
        pick = lax.rem(low + b, planes)
        return jnp.where(z < z_half, pick, planes - 1 - pick)

    order = [plane_at(b) for b in range(planes)]

    def across(p):
        return (p // z_half) != (z // z_half)

    def up_of(p):
        return send(p * PLANE + q, p, 0, 0, me + PLANE)

    def down_of(p):
        return send(p * PLANE + q, p, 1, 0, me - PLANE)

    def to_x(p):
        return send(p * PLANE + q, p, 2, 1, z * PLANE + x_peer)

    def to_y(p):
        return send(p * PLANE + q, p, 3, 2, z * PLANE + y_peer)

    def relay_y(p):
        return send(p * PLANE + x_peer, p, 4, 3, z * PLANE + y_peer, 0, half)

    def relay_x(p):
        return send(p * PLANE + y_peer, p, 5, 4, z * PLANE + x_peer, half, half)

    def wait_in(p, position, kind, first=0, count=None):
        count = rows if count is None else count
        part = gathered.at[p * PLANE + position, pl.ds(first, count)]
        pltpu.make_async_copy(part, part, ag_recv.at[p, kind]).wait()

    def column_stage(d):
        @pl.when(z - d >= 0)
        def _():
            wait_in(z - d, q, 0)

            @pl.when(z < planes - 1)
            def _():
                up_of(z - d).start()

        @pl.when(z + d < planes)
        def _():
            wait_in(z + d, q, 0)

            @pl.when(z > 0)
            def _():
                down_of(z + d).start()

    def spread_stage(p):
        to_x(p).start()
        to_y(p).start()

    def relay_stage(p):
        wait_in(p, x_peer, 1)
        relay_y(p).start()
        wait_in(p, y_peer, 2)
        relay_x(p).start()

    def diagonal_stage(p):
        wait_in(p, d_peer, 3, 0, half)
        wait_in(p, d_peer, 4, half, half)

    def return_copy(group):
        return pltpu.make_async_remote_copy(
            src_ref=outgoing.at[group], dst_ref=incoming.at[me],
            send_sem=ret_send.at[group], recv_sem=ret_recv.at[me],
            device_id={"expert": group}, device_id_type=pl.DeviceIdType.MESH,
        )

    def own_return():
        return pltpu.make_async_copy(outgoing.at[me], incoming.at[me], local_sem)

    batch_tokens = PLANE * rows
    batch_rows = PLANE * pad
    t_i = lax.broadcasted_iota(jnp.int32, (batch_tokens, batch_tokens), 0)
    t_j = lax.broadcasted_iota(jnp.int32, (batch_tokens, batch_tokens), 1)
    before = ((t_j < t_i) & (t_j // rows == t_i // rows)).astype(jnp.bfloat16)
    lane = lax.broadcasted_iota(jnp.int32, (batch_tokens, batch_rows), 1).astype(jnp.float32)
    base = (
        lax.broadcasted_iota(jnp.int32, (batch_tokens, batch_rows), 0) // rows * pad
    ).astype(jnp.float32)
    me_f = me.astype(jnp.float32)
    ff_tile = tile_of(hidden, 256)
    d_tile = tile_of(depth, 512)

    def compute(p, first):
        ids = gathered[pl.ds(p * PLANE, PLANE), :, depth:].reshape(batch_tokens, LANES)
        hit = jnp.sum((ids.astype(jnp.float32) == me_f).astype(jnp.float32), axis=1, keepdims=True)
        pos = jnp.dot(
            before, jnp.broadcast_to(hit, (batch_tokens, batch_rows)).astype(jnp.bfloat16),
            preferred_element_type=jnp.float32,
        )
        kept = (hit > 0.5) & (pos < cap - 0.5)
        chosen = (kept & (lane == base + pos)).astype(jnp.float32)
        chosen_count = chosen
        chosen = chosen.astype(jnp.bfloat16)

        @pl.loop(0, depth // d_tile)
        def _(i):
            cols = pl.ds(pl.multiple_of(i * d_tile, d_tile), d_tile)
            block = gathered[pl.ds(p * PLANE, PLANE), :, cols].reshape(batch_tokens, d_tile)
            packed[:, cols] = lax.dot_general(
                chosen, block, (((0,), (0,)), ((), ())), preferred_element_type=jnp.float32
            ).astype(jnp.bfloat16)

        if first:
            weight_copies[0].wait()
            weight_copies[1].wait()

        @pl.loop(0, hidden // ff_tile)
        def _(i):
            cols = pl.ds(pl.multiple_of(i * ff_tile, ff_tile), ff_tile)
            gate = jnp.dot(packed[...], wg[:, cols], preferred_element_type=jnp.float32)
            up = jnp.dot(packed[...], wu[:, cols], preferred_element_type=jnp.float32)
            mid[:, cols] = (gate / (1.0 + jnp.exp(-gate)) * up).astype(jnp.bfloat16)

        if first:
            weight_copies[2].wait()

        @pl.loop(0, depth // d_tile)
        def _(i):
            cols = pl.ds(pl.multiple_of(i * d_tile, d_tile), d_tile)
            out = jnp.dot(mid[...], wd[:, cols], preferred_element_type=jnp.float32)
            outgoing[pl.ds(p * PLANE, PLANE), :, :, cols] = out.reshape(
                PLANE, outgoing.shape[1], outgoing.shape[2], d_tile
            ).astype(jnp.bfloat16)

        return jnp.sum(chosen_count)

    def give_back(p):
        for j in range(PLANE):
            group = p * PLANE + j

            @pl.when(group != me)
            def _():
                return_copy(group).start()

            @pl.when(group == me)
            def _():
                own_return().start()

    accepted = jnp.float32(0.0)

    @pl.when(z < planes - 1)
    def _():
        up_of(z).start()

    @pl.when(z > 0)
    def _():
        down_of(z).start()

    spread_stage(order[0])
    column_stage(1)
    spread_stage(order[1])
    relay_stage(order[0])
    for d in range(2, planes - 1):
        column_stage(d)
    for b in range(planes):
        if b == 1:
            column_stage(planes - 1)
        if 0 < b < planes - 1:
            spread_stage(order[b + 1])
        diagonal_stage(order[b])
        accepted += compute(order[b], b == 0)
        if b < planes - 1:

            @pl.when(across(order[b]))
            def _():
                give_back(order[b])

            relay_stage(order[b + 1])
        else:
            give_back(order[b])
        if b == planes - 2:
            for c in range(planes - 1):

                @pl.when(jnp.logical_not(across(order[c])))
                def _():
                    give_back(order[c])

    load_ref[0] = accepted * (n / (rows * n * top))

    g_high = gates_ref[...].astype(jnp.bfloat16)
    g_rest = gates_ref[...] - g_high.astype(jnp.float32)
    g_middle = g_rest.astype(jnp.bfloat16)
    g_low = (g_rest - g_middle.astype(jnp.float32)).astype(jnp.bfloat16)
    gate_cols = turned(g_high) + (turned(g_middle) + turned(g_low))
    own_lane = lax.broadcasted_iota(jnp.int32, (rows, LANES), 1).astype(jnp.float32)
    slots = [slot_cols[:, k : k + 1] for k in range(top)]
    hits = functools.reduce(jnp.add, [(s == own_lane).astype(jnp.float32) for s in slots])
    r_i = lax.broadcasted_iota(jnp.int32, (rows, rows), 0)
    r_j = lax.broadcasted_iota(jnp.int32, (rows, rows), 1)
    positions = jnp.dot(
        (r_j < r_i).astype(jnp.bfloat16), hits.astype(jnp.bfloat16),
        preferred_element_type=jnp.float32,
    )
    columns, weights = [], []
    for k in range(top):
        at = jnp.sum(jnp.where(slots[k] == own_lane, positions, 0.0), axis=1, keepdims=True)
        columns.append(slots[k] * pad + at)
        weights.append(jnp.where(at < cap - 0.5, gate_cols[:, k : k + 1], 0.0))
    col_lane = lax.broadcasted_iota(jnp.int32, (rows, batch_rows), 1).astype(jnp.float32)

    for step in range(planes):
        turn = lax.rem(z // z_half + 1 + step // z_half, 2)
        turn = 1 - turn
        inner = step % z_half
        p = turn * z_half + jnp.where(turn == 0, z_half - 1 - inner, inner)
        for j in range(PLANE):
            source = p * PLANE + j

            @pl.when(source != me)
            def _():
                block = incoming.at[source]
                pltpu.make_async_copy(block, block, ret_recv.at[source]).wait()

            @pl.when(source == me)
            def _():
                own_return().wait()

        shift = (p * batch_rows).astype(jnp.float32)
        share = functools.reduce(
            jnp.add,
            [jnp.where(c - shift == col_lane, w, 0.0) for c, w in zip(columns, weights)],
        )
        high = share.astype(jnp.bfloat16)
        rest = share - high.astype(jnp.float32)
        middle = rest.astype(jnp.bfloat16)
        low = (rest - middle.astype(jnp.float32)).astype(jnp.bfloat16)
        spread = jnp.concatenate([high, middle, low], axis=0)

        @pl.loop(0, depth // d_tile)
        def _(i):
            cols = pl.ds(pl.multiple_of(i * d_tile, d_tile), d_tile)
            block = incoming[pl.ds(p * PLANE, PLANE), :, :, cols].astype(jnp.float32)
            block = block.reshape(batch_rows, d_tile).astype(jnp.bfloat16)
            sums = jnp.dot(spread, block, preferred_element_type=jnp.float32)
            sums = sums[:rows] + (sums[rows : 2 * rows] + sums[2 * rows :])
            if step > 0:
                sums = acc[:, cols] + sums
            if step < planes - 1:
                acc[:, cols] = sums
            else:
                mixed_ref[:, cols] = sums.astype(jnp.bfloat16)

    for b in range(planes):
        p = order[b]

        @pl.when((p <= z) & (z < planes - 1))
        def _():
            up_of(p).wait_send()

        @pl.when((p >= z) & (z > 0))
        def _():
            down_of(p).wait_send()

        to_x(p).wait_send()
        to_y(p).wait_send()
        relay_y(p).wait_send()
        relay_x(p).wait_send()
        for j in range(PLANE):
            group = p * PLANE + j

            @pl.when(group != me)
            def _():
                return_copy(group).wait_send()


def per_device_gathered(
    tokens, expert_ids, gate_weights, placement_table, replica_choice, w_gate, w_up, w_down
):
    n = lax.axis_size("expert")
    rows, top = expert_ids.shape
    depth = tokens.shape[1]
    hidden = w_gate.shape[2]
    cap = 5 * rows * top // (4 * n) + 1
    slabs = -(-cap // 8)
    planes = n // PLANE
    bf16, f32 = jnp.bfloat16, jnp.float32
    anywhere = pl.BlockSpec(memory_space=pl.ANY)
    vmem = pl.BlockSpec(memory_space=pltpu.VMEM)
    smem = pl.BlockSpec(memory_space=pltpu.SMEM)
    mixed, load = pl.pallas_call(
        functools.partial(kernel, n, rows, top, cap, depth, hidden),
        out_shape=(
            jax.ShapeDtypeStruct((rows, depth), bf16),
            jax.ShapeDtypeStruct((1,), f32),
        ),
        in_specs=[smem, anywhere, vmem, vmem, vmem, anywhere, anywhere, anywhere],
        out_specs=(vmem, smem),
        scratch_shapes=[
            pltpu.VMEM((n, rows, depth + LANES), bf16),
            pltpu.VMEM((depth, hidden), bf16),
            pltpu.VMEM((depth, hidden), bf16),
            pltpu.VMEM((hidden, depth), bf16),
            pltpu.VMEM((PLANE * slabs * 8, depth), bf16),
            pltpu.VMEM((PLANE * slabs * 8, hidden), bf16),
            pltpu.VMEM((n, slabs, 8, depth), bf16),
            pltpu.VMEM((n, slabs, 8, depth), bf16),
            pltpu.VMEM((rows, depth), f32),
            pltpu.SemaphoreType.DMA((3,)),
            pltpu.SemaphoreType.DMA,
            pltpu.SemaphoreType.DMA((planes, 6)),
            pltpu.SemaphoreType.DMA((planes, 5)),
            pltpu.SemaphoreType.DMA((n,)),
            pltpu.SemaphoreType.DMA((n,)),
            pltpu.SemaphoreType.DMA,
        ],
        compiler_params=pltpu.CompilerParams(
            collective_id=0, has_side_effects=True, vmem_limit_bytes=VMEM_BYTES
        ),
    )(
        placement_table.T, tokens, expert_ids.T, replica_choice.T, gate_weights.T,
        w_gate, w_up, w_down,
    )
    return mixed, load


def solution(mesh):
    placed = (
        P(("dp", "expert"), None),
        P(("dp", "expert"), None),
        P(("dp", "expert"), None),
        P("dp", None),
        P(("dp", "expert"), None),
        P("expert", None, None),
        P("expert", None, None),
        P("expert", None, None),
    )

    def per_device(*args):
        n = mesh.shape["expert"]
        rows, depth = args[0].shape
        weights = 3 * args[5].size
        blocks = n * rows * (depth + LANES) + 2 * n * (rows + 8) * depth
        fits = 2 * (weights + blocks) < 3 * VMEM_BYTES // 4
        if fits and n % (2 * PLANE) == 0 and n <= LANES and rows % 16 == 0:
            return per_device_gathered(*args)
        return per_device_exchange(*args)

    return jax.shard_map(
        per_device,
        mesh=mesh,
        in_specs=placed,
        out_specs=(P(("dp", "expert"), None), P(("dp", "expert"))),
        check_vma=False,
    )
```

```python
import functools

import jax
import jax.numpy as jnp
from jax import lax
from jax.experimental import pallas as pl
from jax.experimental.pallas import tpu as pltpu
from jax.sharding import PartitionSpec as P

PLANE = 4
LANES = 128
VMEM_BYTES = 64 * 1000 * 1000


def run_experts(received, gate_w, up_w, down_w):
    peers, capacity, hidden_dimension = received.shape
    rows = received.reshape(peers * capacity, hidden_dimension)
    gate_part = jnp.dot(rows, gate_w, preferred_element_type=jnp.float32)
    up_part = jnp.dot(rows, up_w, preferred_element_type=jnp.float32)
    hidden = (jax.nn.silu(gate_part) * up_part).astype(jnp.bfloat16)
    output = jnp.dot(hidden, down_w, preferred_element_type=jnp.float32).astype(jnp.bfloat16)
    return output.reshape(peers, capacity, hidden_dimension)


def per_device_exchange(
    tokens, expert_ids, gate_weights, placement_table, replica_choice, w_gate, w_up, w_down
):
    devices = lax.axis_size("expert")
    tok_rows, top_count = expert_ids.shape
    hidden_dimension = tokens.shape[1]
    slot_total = devices
    capacity = 5 * tok_rows * top_count // (4 * slot_total) + 1
    slot_ids = placement_table[expert_ids, replica_choice].astype(jnp.int32).reshape(-1)
    onehot = (slot_ids[:, None] == jnp.arange(slot_total, dtype=jnp.int32)[None, :]).astype(
        jnp.int32
    )
    running = jnp.cumsum(onehot, axis=0)
    position = jnp.sum(running * onehot, axis=1) - 1
    retained_selector = position < capacity
    table_rows = slot_total * capacity
    flat = jnp.where(retained_selector, slot_ids * capacity + position, table_rows)
    token_index = jnp.arange(tok_rows * top_count, dtype=jnp.int32) // top_count
    source_item_index = (
        jnp.full((table_rows,), tok_rows, jnp.int32).at[flat].set(token_index, mode="drop")
    )
    padded = jnp.concatenate([tokens, jnp.zeros((1, hidden_dimension), tokens.dtype)], axis=0)
    outgoing = padded[source_item_index].reshape(devices, capacity, hidden_dimension)
    incoming = lax.all_to_all(outgoing, "expert", split_axis=0, concat_axis=0, tiled=True)
    results = run_experts(incoming, w_gate[0], w_up[0], w_down[0])
    returned = lax.all_to_all(results, "expert", split_axis=0, concat_axis=0, tiled=True)
    returned = returned.reshape(table_rows, hidden_dimension)
    pair_rows = returned[jnp.minimum(flat, table_rows - 1)].reshape(
        tok_rows, top_count, hidden_dimension
    )
    weights = jnp.where(retained_selector.reshape(tok_rows, top_count), gate_weights, 0.0).astype(
        jnp.float32
    )
    mixed = jnp.sum(weights[:, :, None] * pair_rows.astype(jnp.float32), axis=1).astype(
        jnp.bfloat16
    )
    counts = jnp.sum(onehot * retained_selector.astype(jnp.int32)[:, None], axis=0).astype(
        jnp.float32
    )
    own_counts = lax.psum_scatter(counts, "expert", scatter_dimension=0, tiled=True)
    slot_load = own_counts * (slot_total / (tok_rows * devices * top_count))
    return (mixed, slot_load)


def tile_of(size, wanted):
    tile = min(size, wanted)
    while size % tile:
        tile -= LANES
    return tile


def kernel(
    n, rows, top, cap, depth, hidden,
    table_ref, tokens_hbm, ids_ref, choice_ref, gates_ref, wg_hbm, wu_hbm, wd_hbm,
    mixed_ref, load_ref,
    gathered, wg, wu, wd, packed, mid, outgoing, incoming, acc,
    w_sem, own_sem, ag_send, ag_recv, ret_send, ret_recv, local_sem,
):
    planes = n // PLANE
    pad = outgoing.shape[1] * outgoing.shape[2]
    me = lax.axis_index("expert")
    z = me // PLANE
    q = me % PLANE
    y, x = q // 2, q % 2
    x_peer = y * 2 + (1 - x)
    y_peer = (1 - y) * 2 + x
    d_peer = (1 - y) * 2 + (1 - x)
    half = rows // 2

    weight_copies = [
        pltpu.make_async_copy(src.at[0], dst, w_sem.at[i])
        for i, (src, dst) in enumerate(((wg_hbm, wg), (wu_hbm, wu), (wd_hbm, wd)))
    ]
    own = pltpu.make_async_copy(tokens_hbm, gathered.at[me, :, pl.ds(0, depth)], own_sem)
    own.start()
    slot_rows = jnp.zeros((top, rows), jnp.int32)
    for e in range(table_ref.shape[1]):
        pair = jnp.where(choice_ref[...] == 0, table_ref[0, e], table_ref[1, e])
        slot_rows = jnp.where(ids_ref[...] == e, pair, slot_rows)
    eye = (
        lax.broadcasted_iota(jnp.int32, (top, LANES), 0)
        == lax.broadcasted_iota(jnp.int32, (top, LANES), 1)
    ).astype(jnp.bfloat16)

    def turned(block):
        return lax.dot_general(
            block, eye, (((0,), (0,)), ((), ())), preferred_element_type=jnp.float32
        )

    slot_cols = turned(slot_rows.astype(jnp.float32).astype(jnp.bfloat16))
    k_lane = lax.broadcasted_iota(jnp.int32, (rows, LANES), 1)
    gathered[me, :, depth:] = jnp.where(k_lane < top, slot_cols, -1.0).astype(jnp.bfloat16)
    for copy in weight_copies:
        copy.start()

    barrier = pltpu.get_barrier_semaphore()
    for other in range(1, n):
        pl.semaphore_signal(
            barrier, inc=1, device_id={"expert": lax.rem(me + other, n)},
            device_id_type=pl.DeviceIdType.MESH,
        )
    pl.semaphore_wait(barrier, n - 1)
    own.wait()

    def send(group, plane, kind_send, kind_recv, target, first=0, count=None):
        count = rows if count is None else count
        part = gathered.at[group, pl.ds(first, count)]
        return pltpu.make_async_remote_copy(
            src_ref=part, dst_ref=part,
            send_sem=ag_send.at[plane, kind_send], recv_sem=ag_recv.at[plane, kind_recv],
            device_id={"expert": target}, device_id_type=pl.DeviceIdType.MESH,
        )

    z_half = planes // 2
    low = jnp.minimum(z, planes - 1 - z)

    def plane_at(b):
        pick = lax.rem(low + b, planes)
        return jnp.where(z < z_half, pick, planes - 1 - pick)

    order = [plane_at(b) for b in range(planes)]

    def across(p):
        return (p // z_half) != (z // z_half)

    def up_of(p):
        return send(p * PLANE + q, p, 0, 0, me + PLANE)

    def down_of(p):
        return send(p * PLANE + q, p, 1, 0, me - PLANE)

    def to_x(p):
        return send(p * PLANE + q, p, 2, 1, z * PLANE + x_peer)

    def to_y(p):
        return send(p * PLANE + q, p, 3, 2, z * PLANE + y_peer)

    def relay_y(p):
        return send(p * PLANE + x_peer, p, 4, 3, z * PLANE + y_peer, 0, half)

    def relay_x(p):
        return send(p * PLANE + y_peer, p, 5, 4, z * PLANE + x_peer, half, half)

    def wait_in(p, position, kind, first=0, count=None):
        count = rows if count is None else count
        part = gathered.at[p * PLANE + position, pl.ds(first, count)]
        pltpu.make_async_copy(part, part, ag_recv.at[p, kind]).wait()

    def column_stage(d):
        @pl.when(z - d >= 0)
        def _():
            wait_in(z - d, q, 0)

            @pl.when(z < planes - 1)
            def _():
                up_of(z - d).start()

        @pl.when(z + d < planes)
        def _():
            wait_in(z + d, q, 0)

            @pl.when(z > 0)
            def _():
                down_of(z + d).start()

    def spread_stage(p):
        to_x(p).start()
        to_y(p).start()

    def relay_stage(p):
        wait_in(p, x_peer, 1)
        relay_y(p).start()
        wait_in(p, y_peer, 2)
        relay_x(p).start()

    def diagonal_stage(p):
        wait_in(p, d_peer, 3, 0, half)
        wait_in(p, d_peer, 4, half, half)

    def return_copy(group):
        return pltpu.make_async_remote_copy(
            src_ref=outgoing.at[group], dst_ref=incoming.at[me],
            send_sem=ret_send.at[group], recv_sem=ret_recv.at[me],
            device_id={"expert": group}, device_id_type=pl.DeviceIdType.MESH,
        )

    def own_return():
        return pltpu.make_async_copy(outgoing.at[me], incoming.at[me], local_sem)

    batch_tokens = PLANE * rows
    batch_rows = PLANE * pad
    t_i = lax.broadcasted_iota(jnp.int32, (batch_tokens, batch_tokens), 0)
    t_j = lax.broadcasted_iota(jnp.int32, (batch_tokens, batch_tokens), 1)
    before = ((t_j < t_i) & (t_j // rows == t_i // rows)).astype(jnp.bfloat16)
    lane = lax.broadcasted_iota(jnp.int32, (batch_tokens, batch_rows), 1).astype(jnp.float32)
    base = (
        lax.broadcasted_iota(jnp.int32, (batch_tokens, batch_rows), 0) // rows * pad
    ).astype(jnp.float32)
    me_f = me.astype(jnp.float32)
    ff_tile = tile_of(hidden, 256)
    d_tile = tile_of(depth, 512)

    def compute(p, first):
        ids = gathered[pl.ds(p * PLANE, PLANE), :, depth:].reshape(batch_tokens, LANES)
        hit = jnp.sum((ids.astype(jnp.float32) == me_f).astype(jnp.float32), axis=1, keepdims=True)
        pos = jnp.dot(
            before, jnp.broadcast_to(hit, (batch_tokens, batch_rows)).astype(jnp.bfloat16),
            preferred_element_type=jnp.float32,
        )
        kept = (hit > 0.5) & (pos < cap - 0.5)
        chosen = (kept & (lane == base + pos)).astype(jnp.float32)
        chosen_count = chosen
        chosen = chosen.astype(jnp.bfloat16)

        @pl.loop(0, depth // d_tile)
        def _(i):
            cols = pl.ds(pl.multiple_of(i * d_tile, d_tile), d_tile)
            block = gathered[pl.ds(p * PLANE, PLANE), :, cols].reshape(batch_tokens, d_tile)
            packed[:, cols] = lax.dot_general(
                chosen, block, (((0,), (0,)), ((), ())), preferred_element_type=jnp.float32
            ).astype(jnp.bfloat16)

        if first:
            weight_copies[0].wait()
            weight_copies[1].wait()

        @pl.loop(0, hidden // ff_tile)
        def _(i):
            cols = pl.ds(pl.multiple_of(i * ff_tile, ff_tile), ff_tile)
            gate = jnp.dot(packed[...], wg[:, cols], preferred_element_type=jnp.float32)
            up = jnp.dot(packed[...], wu[:, cols], preferred_element_type=jnp.float32)
            mid[:, cols] = (gate / (1.0 + jnp.exp(-gate)) * up).astype(jnp.bfloat16)

        if first:
            weight_copies[2].wait()

        @pl.loop(0, depth // d_tile)
        def _(i):
            cols = pl.ds(pl.multiple_of(i * d_tile, d_tile), d_tile)
            out = jnp.dot(mid[...], wd[:, cols], preferred_element_type=jnp.float32)
            outgoing[pl.ds(p * PLANE, PLANE), :, :, cols] = out.reshape(
                PLANE, outgoing.shape[1], outgoing.shape[2], d_tile
            ).astype(jnp.bfloat16)

        return jnp.sum(chosen_count)

    def give_back(p):
        for j in range(PLANE):
            group = p * PLANE + j

            @pl.when(group != me)
            def _():
                return_copy(group).start()

            @pl.when(group == me)
            def _():
                own_return().start()

    accepted = jnp.float32(0.0)

    @pl.when(z < planes - 1)
    def _():
        up_of(z).start()

    @pl.when(z > 0)
    def _():
        down_of(z).start()

    spread_stage(order[0])
    column_stage(1)
    spread_stage(order[1])
    relay_stage(order[0])
    column_stage(2)
    relay_stage(order[1])
    spread_stage(order[2])
    turns = [1, 0] + list(range(2, planes))
    for i, b in enumerate(turns):
        diagonal_stage(order[b])
        accepted += compute(order[b], i == 0)

        @pl.when(across(order[b]))
        def _():
            give_back(order[b])

        if i + 3 < planes:
            column_stage(i + 3)
            relay_stage(order[i + 2])
            spread_stage(order[i + 3])
        elif i + 2 < planes:
            relay_stage(order[i + 2])

    for b in turns:

        @pl.when(jnp.logical_not(across(order[b])))
        def _():
            give_back(order[b])

    load_ref[0] = accepted * (n / (rows * n * top))

    g_high = gates_ref[...].astype(jnp.bfloat16)
    g_rest = gates_ref[...] - g_high.astype(jnp.float32)
    g_middle = g_rest.astype(jnp.bfloat16)
    g_low = (g_rest - g_middle.astype(jnp.float32)).astype(jnp.bfloat16)
    gate_cols = turned(g_high) + (turned(g_middle) + turned(g_low))
    own_lane = lax.broadcasted_iota(jnp.int32, (rows, LANES), 1).astype(jnp.float32)
    slots = [slot_cols[:, k : k + 1] for k in range(top)]
    hits = functools.reduce(jnp.add, [(s == own_lane).astype(jnp.float32) for s in slots])
    r_i = lax.broadcasted_iota(jnp.int32, (rows, rows), 0)
    r_j = lax.broadcasted_iota(jnp.int32, (rows, rows), 1)
    positions = jnp.dot(
        (r_j < r_i).astype(jnp.bfloat16), hits.astype(jnp.bfloat16),
        preferred_element_type=jnp.float32,
    )
    columns, weights = [], []
    for k in range(top):
        at = jnp.sum(jnp.where(slots[k] == own_lane, positions, 0.0), axis=1, keepdims=True)
        columns.append(slots[k] * pad + at)
        weights.append(jnp.where(at < cap - 0.5, gate_cols[:, k : k + 1], 0.0))
    col_lane = lax.broadcasted_iota(jnp.int32, (rows, batch_rows), 1).astype(jnp.float32)

    for step in range(planes):
        turn = lax.rem(z // z_half + 1 + step // z_half, 2)
        turn = 1 - turn
        inner = step % z_half
        p = turn * z_half + jnp.where(turn == 0, z_half - 1 - inner, inner)
        for j in range(PLANE):
            source = p * PLANE + j

            @pl.when(source != me)
            def _():
                block = incoming.at[source]
                pltpu.make_async_copy(block, block, ret_recv.at[source]).wait()

            @pl.when(source == me)
            def _():
                own_return().wait()

        shift = (p * batch_rows).astype(jnp.float32)
        share = functools.reduce(
            jnp.add,
            [jnp.where(c - shift == col_lane, w, 0.0) for c, w in zip(columns, weights)],
        )
        high = share.astype(jnp.bfloat16)
        rest = share - high.astype(jnp.float32)
        middle = rest.astype(jnp.bfloat16)
        low = (rest - middle.astype(jnp.float32)).astype(jnp.bfloat16)
        spread = jnp.concatenate([high, middle, low], axis=0)

        @pl.loop(0, depth // d_tile)
        def _(i):
            cols = pl.ds(pl.multiple_of(i * d_tile, d_tile), d_tile)
            block = incoming[pl.ds(p * PLANE, PLANE), :, :, cols].astype(jnp.float32)
            block = block.reshape(batch_rows, d_tile).astype(jnp.bfloat16)
            sums = jnp.dot(spread, block, preferred_element_type=jnp.float32)
            sums = sums[:rows] + (sums[rows : 2 * rows] + sums[2 * rows :])
            if step > 0:
                sums = acc[:, cols] + sums
            if step < planes - 1:
                acc[:, cols] = sums
            else:
                mixed_ref[:, cols] = sums.astype(jnp.bfloat16)

    for b in range(planes):
        p = order[b]

        @pl.when((p <= z) & (z < planes - 1))
        def _():
            up_of(p).wait_send()

        @pl.when((p >= z) & (z > 0))
        def _():
            down_of(p).wait_send()

        to_x(p).wait_send()
        to_y(p).wait_send()
        relay_y(p).wait_send()
        relay_x(p).wait_send()
        for j in range(PLANE):
            group = p * PLANE + j

            @pl.when(group != me)
            def _():
                return_copy(group).wait_send()


def per_device_gathered(
    tokens, expert_ids, gate_weights, placement_table, replica_choice, w_gate, w_up, w_down
):
    n = lax.axis_size("expert")
    rows, top = expert_ids.shape
    depth = tokens.shape[1]
    hidden = w_gate.shape[2]
    cap = 5 * rows * top // (4 * n) + 1
    slabs = -(-cap // 8)
    planes = n // PLANE
    bf16, f32 = jnp.bfloat16, jnp.float32
    anywhere = pl.BlockSpec(memory_space=pl.ANY)
    vmem = pl.BlockSpec(memory_space=pltpu.VMEM)
    smem = pl.BlockSpec(memory_space=pltpu.SMEM)
    mixed, load = pl.pallas_call(
        functools.partial(kernel, n, rows, top, cap, depth, hidden),
        out_shape=(
            jax.ShapeDtypeStruct((rows, depth), bf16),
            jax.ShapeDtypeStruct((1,), f32),
        ),
        in_specs=[smem, anywhere, vmem, vmem, vmem, anywhere, anywhere, anywhere],
        out_specs=(vmem, smem),
        scratch_shapes=[
            pltpu.VMEM((n, rows, depth + LANES), bf16),
            pltpu.VMEM((depth, hidden), bf16),
            pltpu.VMEM((depth, hidden), bf16),
            pltpu.VMEM((hidden, depth), bf16),
            pltpu.VMEM((PLANE * slabs * 8, depth), bf16),
            pltpu.VMEM((PLANE * slabs * 8, hidden), bf16),
            pltpu.VMEM((n, slabs, 8, depth), bf16),
            pltpu.VMEM((n, slabs, 8, depth), bf16),
            pltpu.VMEM((rows, depth), f32),
            pltpu.SemaphoreType.DMA((3,)),
            pltpu.SemaphoreType.DMA,
            pltpu.SemaphoreType.DMA((planes, 6)),
            pltpu.SemaphoreType.DMA((planes, 5)),
            pltpu.SemaphoreType.DMA((n,)),
            pltpu.SemaphoreType.DMA((n,)),
            pltpu.SemaphoreType.DMA,
        ],
        compiler_params=pltpu.CompilerParams(
            collective_id=0, has_side_effects=True, vmem_limit_bytes=VMEM_BYTES
        ),
    )(
        placement_table.T, tokens, expert_ids.T, replica_choice.T, gate_weights.T,
        w_gate, w_up, w_down,
    )
    return mixed, load


def solution(mesh):
    placed = (
        P(("dp", "expert"), None),
        P(("dp", "expert"), None),
        P(("dp", "expert"), None),
        P("dp", None),
        P(("dp", "expert"), None),
        P("expert", None, None),
        P("expert", None, None),
        P("expert", None, None),
    )

    def per_device(*args):
        n = mesh.shape["expert"]
        rows, depth = args[0].shape
        weights = 3 * args[5].size
        blocks = n * rows * (depth + LANES) + 2 * n * (rows + 8) * depth
        fits = 2 * (weights + blocks) < 3 * VMEM_BYTES // 4
        if fits and n % (2 * PLANE) == 0 and n > 2 * PLANE and n <= LANES and rows % 16 == 0:
            return per_device_gathered(*args)
        return per_device_exchange(*args)

    return jax.shard_map(
        per_device,
        mesh=mesh,
        in_specs=placed,
        out_specs=(P(("dp", "expert"), None), P(("dp", "expert"))),
        check_vma=False,
    )
```

```python
import functools

import jax
import jax.numpy as jnp
from jax import lax
from jax.experimental import pallas as pl
from jax.experimental.pallas import tpu as pltpu
from jax.sharding import PartitionSpec as P

PLANE = 4
LANES = 128
D_TILE = 256
VMEM_BYTES = 64 * 1000 * 1000


def run_experts(received, gate_w, up_w, down_w):
    peers, capacity, hidden_dimension = received.shape
    rows = received.reshape(peers * capacity, hidden_dimension)
    gate_part = jnp.dot(rows, gate_w, preferred_element_type=jnp.float32)
    up_part = jnp.dot(rows, up_w, preferred_element_type=jnp.float32)
    hidden = (jax.nn.silu(gate_part) * up_part).astype(jnp.bfloat16)
    output = jnp.dot(hidden, down_w, preferred_element_type=jnp.float32).astype(jnp.bfloat16)
    return output.reshape(peers, capacity, hidden_dimension)


def per_device_exchange(
    tokens, expert_ids, gate_weights, placement_table, replica_choice, w_gate, w_up, w_down
):
    devices = lax.axis_size("expert")
    tok_rows, top_count = expert_ids.shape
    hidden_dimension = tokens.shape[1]
    slot_total = devices
    capacity = 5 * tok_rows * top_count // (4 * slot_total) + 1
    slot_ids = placement_table[expert_ids, replica_choice].astype(jnp.int32).reshape(-1)
    onehot = (slot_ids[:, None] == jnp.arange(slot_total, dtype=jnp.int32)[None, :]).astype(
        jnp.int32
    )
    running = jnp.cumsum(onehot, axis=0)
    position = jnp.sum(running * onehot, axis=1) - 1
    retained_selector = position < capacity
    table_rows = slot_total * capacity
    flat = jnp.where(retained_selector, slot_ids * capacity + position, table_rows)
    token_index = jnp.arange(tok_rows * top_count, dtype=jnp.int32) // top_count
    source_item_index = (
        jnp.full((table_rows,), tok_rows, jnp.int32).at[flat].set(token_index, mode="drop")
    )
    padded = jnp.concatenate([tokens, jnp.zeros((1, hidden_dimension), tokens.dtype)], axis=0)
    outgoing = padded[source_item_index].reshape(devices, capacity, hidden_dimension)
    incoming = lax.all_to_all(outgoing, "expert", split_axis=0, concat_axis=0, tiled=True)
    results = run_experts(incoming, w_gate[0], w_up[0], w_down[0])
    returned = lax.all_to_all(results, "expert", split_axis=0, concat_axis=0, tiled=True)
    returned = returned.reshape(table_rows, hidden_dimension)
    pair_rows = returned[jnp.minimum(flat, table_rows - 1)].reshape(
        tok_rows, top_count, hidden_dimension
    )
    weights = jnp.where(retained_selector.reshape(tok_rows, top_count), gate_weights, 0.0).astype(
        jnp.float32
    )
    mixed = jnp.sum(weights[:, :, None] * pair_rows.astype(jnp.float32), axis=1).astype(
        jnp.bfloat16
    )
    counts = jnp.sum(onehot * retained_selector.astype(jnp.int32)[:, None], axis=0).astype(
        jnp.float32
    )
    own_counts = lax.psum_scatter(counts, "expert", scatter_dimension=0, tiled=True)
    slot_load = own_counts * (slot_total / (tok_rows * devices * top_count))
    return (mixed, slot_load)


def tile_of(size, wanted):
    tile = min(size, wanted)
    while size % tile:
        tile -= LANES
    return tile


def folds_of(cap, depth, tile):
    full = cap // 8
    offset, first, pieces = full * depth, full * 8, []
    for count in (4, 2, 1):
        if cap % 8 & count:
            folds = max(f for f in range(1, 8 // count + 1) if depth // tile % f == 0)
            width = depth // folds
            pieces.append((first, count, folds, width, offset))
            first, offset = first + count, offset + width
    return full, pieces, offset


def kernel(
    n, rows, top, cap, depth, hidden,
    table_ref, tokens_hbm, ids_ref, choice_ref, gates_ref, wg_hbm, wu_hbm, wd_hbm,
    mixed_ref, load_ref,
    gathered, wg, wu, wd, packed, mid, outgoing, incoming, acc, folded,
    w_sem, own_sem, ag_send, ag_recv, ret_send, ret_recv, local_sem,
):
    planes = n // PLANE
    pad = packed.shape[0] // PLANE
    d_tile = tile_of(depth, D_TILE)
    full, pieces, _ = folds_of(cap, depth, d_tile)
    me = lax.axis_index("expert")
    z = me // PLANE
    q = me % PLANE
    y, x = q // 2, q % 2
    x_peer = y * 2 + (1 - x)
    y_peer = (1 - y) * 2 + x
    d_peer = (1 - y) * 2 + (1 - x)
    half = rows // 2

    weight_copies = [
        pltpu.make_async_copy(src.at[0], dst, w_sem.at[i])
        for i, (src, dst) in enumerate(((wg_hbm, wg), (wu_hbm, wu), (wd_hbm, wd)))
    ]
    own = pltpu.make_async_copy(tokens_hbm, gathered.at[me, :, pl.ds(0, depth)], own_sem)
    own.start()
    slot_rows = jnp.zeros((top, rows), jnp.int32)
    for e in range(table_ref.shape[1]):
        pair = jnp.where(choice_ref[...] == 0, table_ref[0, e], table_ref[1, e])
        slot_rows = jnp.where(ids_ref[...] == e, pair, slot_rows)
    folded[...] = jnp.zeros_like(folded)
    eye = (
        lax.broadcasted_iota(jnp.int32, (top, LANES), 0)
        == lax.broadcasted_iota(jnp.int32, (top, LANES), 1)
    ).astype(jnp.bfloat16)

    def turned(block):
        return lax.dot_general(
            block, eye, (((0,), (0,)), ((), ())), preferred_element_type=jnp.float32
        )

    slot_cols = turned(slot_rows.astype(jnp.float32).astype(jnp.bfloat16))
    k_lane = lax.broadcasted_iota(jnp.int32, (rows, LANES), 1)
    gathered[me, :, depth:] = jnp.where(k_lane < top, slot_cols, -1.0).astype(jnp.bfloat16)
    for copy in weight_copies:
        copy.start()

    barrier = pltpu.get_barrier_semaphore()
    for other in range(1, n):
        pl.semaphore_signal(
            barrier, inc=1, device_id={"expert": lax.rem(me + other, n)},
            device_id_type=pl.DeviceIdType.MESH,
        )
    pl.semaphore_wait(barrier, n - 1)
    own.wait()

    def send(group, plane, kind_send, kind_recv, target, first=0, count=None):
        count = rows if count is None else count
        part = gathered.at[group, pl.ds(first, count)]
        return pltpu.make_async_remote_copy(
            src_ref=part, dst_ref=part,
            send_sem=ag_send.at[plane, kind_send], recv_sem=ag_recv.at[plane, kind_recv],
            device_id={"expert": target}, device_id_type=pl.DeviceIdType.MESH,
        )

    z_half = planes // 2
    low = jnp.minimum(z, planes - 1 - z)

    def plane_at(b):
        pick = lax.rem(low + b, planes)
        return jnp.where(z < z_half, pick, planes - 1 - pick)

    order = [plane_at(b) for b in range(planes)]

    def across(p):
        return (p // z_half) != (z // z_half)

    def up_of(p):
        return send(p * PLANE + q, p, 0, 0, me + PLANE)

    def down_of(p):
        return send(p * PLANE + q, p, 1, 0, me - PLANE)

    def to_x(p):
        return send(p * PLANE + q, p, 2, 1, z * PLANE + x_peer)

    def to_y(p):
        return send(p * PLANE + q, p, 3, 2, z * PLANE + y_peer)

    def relay_y(p):
        return send(p * PLANE + x_peer, p, 4, 3, z * PLANE + y_peer, 0, half)

    def relay_x(p):
        return send(p * PLANE + y_peer, p, 5, 4, z * PLANE + x_peer, half, half)

    def wait_in(p, position, kind, first=0, count=None):
        count = rows if count is None else count
        part = gathered.at[p * PLANE + position, pl.ds(first, count)]
        pltpu.make_async_copy(part, part, ag_recv.at[p, kind]).wait()

    def column_stage(d):
        @pl.when(z - d >= 0)
        def _():
            wait_in(z - d, q, 0)

            @pl.when(z < planes - 1)
            def _():
                up_of(z - d).start()

        @pl.when(z + d < planes)
        def _():
            wait_in(z + d, q, 0)

            @pl.when(z > 0)
            def _():
                down_of(z + d).start()

    def spread_stage(p):
        to_x(p).start()
        to_y(p).start()

    def relay_stage(p):
        wait_in(p, x_peer, 1)
        relay_y(p).start()
        wait_in(p, y_peer, 2)
        relay_x(p).start()

    def diagonal_stage(p):
        wait_in(p, d_peer, 3, 0, half)
        wait_in(p, d_peer, 4, half, half)

    def return_copy(group):
        return pltpu.make_async_remote_copy(
            src_ref=outgoing.at[group], dst_ref=incoming.at[me],
            send_sem=ret_send.at[group], recv_sem=ret_recv.at[me],
            device_id={"expert": group}, device_id_type=pl.DeviceIdType.MESH,
        )

    def own_return():
        return pltpu.make_async_copy(outgoing.at[me], incoming.at[me], local_sem)

    batch_tokens = PLANE * rows
    batch_rows = PLANE * pad
    t_i = lax.broadcasted_iota(jnp.int32, (batch_tokens, batch_tokens), 0)
    t_j = lax.broadcasted_iota(jnp.int32, (batch_tokens, batch_tokens), 1)
    before = ((t_j < t_i) & (t_j // rows == t_i // rows)).astype(jnp.bfloat16)
    lane = lax.broadcasted_iota(jnp.int32, (batch_tokens, batch_rows), 1).astype(jnp.float32)
    base = (
        lax.broadcasted_iota(jnp.int32, (batch_tokens, batch_rows), 0) // rows * pad
    ).astype(jnp.float32)
    me_f = me.astype(jnp.float32)
    ff_tile = tile_of(hidden, 256)

    def compute(p, first):
        ids = gathered[pl.ds(p * PLANE, PLANE), :, depth:].reshape(batch_tokens, LANES)
        hit = jnp.sum((ids.astype(jnp.float32) == me_f).astype(jnp.float32), axis=1, keepdims=True)
        pos = jnp.dot(
            before, jnp.broadcast_to(hit, (batch_tokens, batch_rows)).astype(jnp.bfloat16),
            preferred_element_type=jnp.float32,
        )
        kept = (hit > 0.5) & (pos < cap - 0.5)
        chosen = (kept & (lane == base + pos)).astype(jnp.float32)
        chosen_count = chosen
        chosen = chosen.astype(jnp.bfloat16)

        @pl.loop(0, depth // d_tile)
        def _(i):
            cols = pl.ds(pl.multiple_of(i * d_tile, d_tile), d_tile)
            block = gathered[pl.ds(p * PLANE, PLANE), :, cols].reshape(batch_tokens, d_tile)
            packed[:, cols] = lax.dot_general(
                chosen, block, (((0,), (0,)), ((), ())), preferred_element_type=jnp.float32
            ).astype(jnp.bfloat16)

        if first:
            weight_copies[0].wait()
            weight_copies[1].wait()

        @pl.loop(0, hidden // ff_tile)
        def _(i):
            cols = pl.ds(pl.multiple_of(i * ff_tile, ff_tile), ff_tile)
            gate = jnp.dot(packed[...], wg[:, cols], preferred_element_type=jnp.float32)
            up = jnp.dot(packed[...], wu[:, cols], preferred_element_type=jnp.float32)
            mid[:, cols] = (gate / (1.0 + jnp.exp(-gate)) * up).astype(jnp.bfloat16)

        if first:
            weight_copies[2].wait()

        @pl.loop(0, depth // d_tile)
        def _(i):
            cols = pl.ds(pl.multiple_of(i * d_tile, d_tile), d_tile)
            out = jnp.dot(mid[...], wd[:, cols], preferred_element_type=jnp.float32)
            out = out.reshape(PLANE, pad, d_tile)
            for slab in range(full):
                at = pl.ds(pl.multiple_of(slab * depth + i * d_tile, d_tile), d_tile)
                outgoing[pl.ds(p * PLANE, PLANE), :, at] = out[
                    :, slab * 8 : slab * 8 + 8
                ].astype(jnp.bfloat16)
            for start, count, _, width, offset in pieces:
                steps = width // d_tile
                at = pl.ds(
                    pl.multiple_of(offset - full * depth + i % steps * d_tile, d_tile), d_tile
                )
                for r in range(count):
                    folded[:, pl.ds(i // steps * count + r, 1), at] = out[
                        :, start + r : start + r + 1
                    ]

        if pieces:
            outgoing[pl.ds(p * PLANE, PLANE), :, full * depth :] = folded[...].astype(
                jnp.bfloat16
            )
        return jnp.sum(chosen_count)

    def give_back(p):
        for j in range(PLANE):
            group = p * PLANE + j

            @pl.when(group != me)
            def _():
                return_copy(group).start()

            @pl.when(group == me)
            def _():
                own_return().start()

    accepted = jnp.float32(0.0)

    @pl.when(z < planes - 1)
    def _():
        up_of(z).start()

    @pl.when(z > 0)
    def _():
        down_of(z).start()

    spread_stage(order[0])
    column_stage(1)
    spread_stage(order[1])
    relay_stage(order[0])
    column_stage(2)
    relay_stage(order[1])
    spread_stage(order[2])
    turns = [1, 0] + list(range(2, planes))
    for i, b in enumerate(turns):
        diagonal_stage(order[b])
        accepted += compute(order[b], i == 0)

        @pl.when(across(order[b]))
        def _():
            give_back(order[b])

        if i + 3 < planes:
            column_stage(i + 3)
            relay_stage(order[i + 2])
            spread_stage(order[i + 3])
        elif i + 2 < planes:
            relay_stage(order[i + 2])

    for b in turns:

        @pl.when(jnp.logical_not(across(order[b])))
        def _():
            give_back(order[b])

    load_ref[0] = accepted * (n / (rows * n * top))

    g_high = gates_ref[...].astype(jnp.bfloat16)
    g_rest = gates_ref[...] - g_high.astype(jnp.float32)
    g_middle = g_rest.astype(jnp.bfloat16)
    g_low = (g_rest - g_middle.astype(jnp.float32)).astype(jnp.bfloat16)
    gate_cols = turned(g_high) + (turned(g_middle) + turned(g_low))
    own_lane = lax.broadcasted_iota(jnp.int32, (rows, LANES), 1).astype(jnp.float32)
    slots = [slot_cols[:, k : k + 1] for k in range(top)]
    hits = functools.reduce(jnp.add, [(s == own_lane).astype(jnp.float32) for s in slots])
    r_i = lax.broadcasted_iota(jnp.int32, (rows, rows), 0)
    r_j = lax.broadcasted_iota(jnp.int32, (rows, rows), 1)
    positions = jnp.dot(
        (r_j < r_i).astype(jnp.bfloat16), hits.astype(jnp.bfloat16),
        preferred_element_type=jnp.float32,
    )
    columns, weights, inside_plane = [], [], []
    for k in range(top):
        at = jnp.sum(jnp.where(slots[k] == own_lane, positions, 0.0), axis=1, keepdims=True)
        lane_of = at + (PLANE * 8 - 8) * jnp.floor(at * 0.125)
        moves = []
        for index, (start, count, _, _, _) in enumerate(pieces):
            inside = (at > start - 0.5) & (at < start + count - 0.5)
            lane_of = jnp.where(inside, (full + index) * PLANE * 8 + at - start, lane_of)
            moves.append(jnp.where(inside, float(count), 0.0))
        columns.append((slots[k] * 8 + lane_of, moves))
        weights.append(jnp.where(at < cap - 0.5, gate_cols[:, k : k + 1], 0.0))
        inside_plane.append(jnp.floor(slots[k] * (1.0 / PLANE)))
    stacked = (full + len(pieces)) * PLANE * 8
    col_lane = lax.broadcasted_iota(jnp.int32, (rows, stacked), 1).astype(jnp.float32)

    for step in range(planes):
        turn = lax.rem(z // z_half + 1 + step // z_half, 2)
        turn = 1 - turn
        inner = step % z_half
        p = turn * z_half + jnp.where(turn == 0, z_half - 1 - inner, inner)
        for j in range(PLANE):
            source = p * PLANE + j

            @pl.when(source != me)
            def _():
                block = incoming.at[source]
                pltpu.make_async_copy(block, block, ret_recv.at[source]).wait()

            @pl.when(source == me)
            def _():
                own_return().wait()

        p_f = p.astype(jnp.float32)
        here = [jnp.where(g == p_f, w, 0.0) for g, w in zip(inside_plane, weights)]

        @pl.loop(0, depth // d_tile)
        def _(i):
            cols = pl.ds(pl.multiple_of(i * d_tile, d_tile), d_tile)
            offsets = [slab * depth + i * d_tile for slab in range(full)]
            shifts = []
            for _, _, _, width, offset in pieces:
                steps = width // d_tile
                offsets.append(offset + i % steps * d_tile)
                shifts.append((i // steps).astype(jnp.float32))
            share = jnp.zeros((rows, stacked), jnp.float32)
            for (lane_of, moves), w in zip(columns, here):
                at = lane_of - p_f * (PLANE * 8)
                for move, shift in zip(moves, shifts):
                    at = at + move * shift
                share = share + jnp.where(at == col_lane, w, 0.0)
            high = share.astype(jnp.bfloat16)
            rest = share - high.astype(jnp.float32)
            middle = rest.astype(jnp.bfloat16)
            low = (rest - middle.astype(jnp.float32)).astype(jnp.bfloat16)
            spread = jnp.concatenate([high, middle, low], axis=0)
            slabs = [
                incoming[
                    pl.ds(p * PLANE, PLANE), :, pl.ds(pl.multiple_of(o, d_tile), d_tile)
                ].astype(jnp.float32).reshape(PLANE * 8, d_tile)
                for o in offsets
            ]
            block = jnp.concatenate(slabs, axis=0).astype(jnp.bfloat16)
            sums = jnp.dot(spread, block, preferred_element_type=jnp.float32)
            sums = sums[:rows] + (sums[rows : 2 * rows] + sums[2 * rows :])
            if step > 0:
                sums = acc[:, cols] + sums
            if step < planes - 1:
                acc[:, cols] = sums
            else:
                mixed_ref[:, cols] = sums.astype(jnp.bfloat16)

    for b in range(planes):
        p = order[b]

        @pl.when((p <= z) & (z < planes - 1))
        def _():
            up_of(p).wait_send()

        @pl.when((p >= z) & (z > 0))
        def _():
            down_of(p).wait_send()

        to_x(p).wait_send()
        to_y(p).wait_send()
        relay_y(p).wait_send()
        relay_x(p).wait_send()
        for j in range(PLANE):
            group = p * PLANE + j

            @pl.when(group != me)
            def _():
                return_copy(group).wait_send()


def per_device_gathered(
    tokens, expert_ids, gate_weights, placement_table, replica_choice, w_gate, w_up, w_down
):
    n = lax.axis_size("expert")
    rows, top = expert_ids.shape
    depth = tokens.shape[1]
    hidden = w_gate.shape[2]
    cap = 5 * rows * top // (4 * n) + 1
    slabs = -(-cap // 8)
    _, _, length = folds_of(cap, depth, tile_of(depth, D_TILE))
    planes = n // PLANE
    bf16, f32 = jnp.bfloat16, jnp.float32
    anywhere = pl.BlockSpec(memory_space=pl.ANY)
    vmem = pl.BlockSpec(memory_space=pltpu.VMEM)
    smem = pl.BlockSpec(memory_space=pltpu.SMEM)
    mixed, load = pl.pallas_call(
        functools.partial(kernel, n, rows, top, cap, depth, hidden),
        out_shape=(
            jax.ShapeDtypeStruct((rows, depth), bf16),
            jax.ShapeDtypeStruct((1,), f32),
        ),
        in_specs=[smem, anywhere, vmem, vmem, vmem, anywhere, anywhere, anywhere],
        out_specs=(vmem, smem),
        scratch_shapes=[
            pltpu.VMEM((n, rows, depth + LANES), bf16),
            pltpu.VMEM((depth, hidden), bf16),
            pltpu.VMEM((depth, hidden), bf16),
            pltpu.VMEM((hidden, depth), bf16),
            pltpu.VMEM((PLANE * slabs * 8, depth), bf16),
            pltpu.VMEM((PLANE * slabs * 8, hidden), bf16),
            pltpu.VMEM((n, 8, length), bf16),
            pltpu.VMEM((n, 8, length), bf16),
            pltpu.VMEM((rows, depth), f32),
            pltpu.VMEM((PLANE, 8, max(length - cap // 8 * depth, LANES)), f32),
            pltpu.SemaphoreType.DMA((3,)),
            pltpu.SemaphoreType.DMA,
            pltpu.SemaphoreType.DMA((planes, 6)),
            pltpu.SemaphoreType.DMA((planes, 5)),
            pltpu.SemaphoreType.DMA((n,)),
            pltpu.SemaphoreType.DMA((n,)),
            pltpu.SemaphoreType.DMA,
        ],
        compiler_params=pltpu.CompilerParams(
            collective_id=0, has_side_effects=True, vmem_limit_bytes=VMEM_BYTES
        ),
    )(
        placement_table.T, tokens, expert_ids.T, replica_choice.T, gate_weights.T,
        w_gate, w_up, w_down,
    )
    return mixed, load


def solution(mesh):
    placed = (
        P(("dp", "expert"), None),
        P(("dp", "expert"), None),
        P(("dp", "expert"), None),
        P("dp", None),
        P(("dp", "expert"), None),
        P("expert", None, None),
        P("expert", None, None),
        P("expert", None, None),
    )

    def per_device(*args):
        n = mesh.shape["expert"]
        rows, depth = args[0].shape
        weights = 3 * args[5].size
        blocks = n * rows * (depth + LANES) + 2 * n * (rows + 8) * depth
        fits = 2 * (weights + blocks) < 3 * VMEM_BYTES // 4
        if fits and n % (2 * PLANE) == 0 and n > 2 * PLANE and n <= LANES and rows % 16 == 0:
            return per_device_gathered(*args)
        return per_device_exchange(*args)

    return jax.shard_map(
        per_device,
        mesh=mesh,
        in_specs=placed,
        out_specs=(P(("dp", "expert"), None), P(("dp", "expert"))),
        check_vma=False,
    )
```

```python
import functools

import jax
import jax.numpy as jnp
from jax import lax
from jax.experimental import pallas as pl
from jax.experimental.pallas import tpu as pltpu
from jax.sharding import PartitionSpec as P

PLANE = 4
LANES = 128
D_TILE = 256
VMEM_BYTES = 64 * 1000 * 1000


def run_experts(received, gate_w, up_w, down_w):
    peers, capacity, hidden_dimension = received.shape
    rows = received.reshape(peers * capacity, hidden_dimension)
    gate_part = jnp.dot(rows, gate_w, preferred_element_type=jnp.float32)
    up_part = jnp.dot(rows, up_w, preferred_element_type=jnp.float32)
    hidden = (jax.nn.silu(gate_part) * up_part).astype(jnp.bfloat16)
    output = jnp.dot(hidden, down_w, preferred_element_type=jnp.float32).astype(jnp.bfloat16)
    return output.reshape(peers, capacity, hidden_dimension)


def per_device_exchange(
    tokens, expert_ids, gate_weights, placement_table, replica_choice, w_gate, w_up, w_down
):
    devices = lax.axis_size("expert")
    tok_rows, top_count = expert_ids.shape
    hidden_dimension = tokens.shape[1]
    slot_total = devices
    capacity = 5 * tok_rows * top_count // (4 * slot_total) + 1
    slot_ids = placement_table[expert_ids, replica_choice].astype(jnp.int32).reshape(-1)
    onehot = (slot_ids[:, None] == jnp.arange(slot_total, dtype=jnp.int32)[None, :]).astype(
        jnp.int32
    )
    running = jnp.cumsum(onehot, axis=0)
    position = jnp.sum(running * onehot, axis=1) - 1
    retained_selector = position < capacity
    table_rows = slot_total * capacity
    flat = jnp.where(retained_selector, slot_ids * capacity + position, table_rows)
    token_index = jnp.arange(tok_rows * top_count, dtype=jnp.int32) // top_count
    source_item_index = (
        jnp.full((table_rows,), tok_rows, jnp.int32).at[flat].set(token_index, mode="drop")
    )
    padded = jnp.concatenate([tokens, jnp.zeros((1, hidden_dimension), tokens.dtype)], axis=0)
    outgoing = padded[source_item_index].reshape(devices, capacity, hidden_dimension)
    incoming = lax.all_to_all(outgoing, "expert", split_axis=0, concat_axis=0, tiled=True)
    results = run_experts(incoming, w_gate[0], w_up[0], w_down[0])
    returned = lax.all_to_all(results, "expert", split_axis=0, concat_axis=0, tiled=True)
    returned = returned.reshape(table_rows, hidden_dimension)
    pair_rows = returned[jnp.minimum(flat, table_rows - 1)].reshape(
        tok_rows, top_count, hidden_dimension
    )
    weights = jnp.where(retained_selector.reshape(tok_rows, top_count), gate_weights, 0.0).astype(
        jnp.float32
    )
    mixed = jnp.sum(weights[:, :, None] * pair_rows.astype(jnp.float32), axis=1).astype(
        jnp.bfloat16
    )
    counts = jnp.sum(onehot * retained_selector.astype(jnp.int32)[:, None], axis=0).astype(
        jnp.float32
    )
    own_counts = lax.psum_scatter(counts, "expert", scatter_dimension=0, tiled=True)
    slot_load = own_counts * (slot_total / (tok_rows * devices * top_count))
    return (mixed, slot_load)


def tile_of(size, wanted):
    tile = min(size, wanted)
    while size % tile:
        tile -= LANES
    return tile


def folds_of(cap, depth, tile):
    full = cap // 8
    offset, first, pieces = full * depth, full * 8, []
    for count in (4, 2, 1):
        if cap % 8 & count:
            folds = max(f for f in range(1, 8 // count + 1) if depth // tile % f == 0)
            width = depth // folds
            pieces.append((first, count, folds, width, offset))
            first, offset = first + count, offset + width
    return full, pieces, offset


def kernel(
    n, rows, top, cap, depth, hidden,
    table_ref, tokens_hbm, ids_ref, choice_ref, gates_ref, wg_hbm, wu_hbm, wd_hbm,
    mixed_ref, load_ref,
    gathered, wg, wu, wd, packed, mid, outgoing, incoming, acc, folded, spreads,
    w_sem, own_sem, ag_send, ag_recv, ret_send, ret_recv, local_sem,
):
    planes = n // PLANE
    pad = packed.shape[0] // PLANE
    d_tile = tile_of(depth, D_TILE)
    full, pieces, _ = folds_of(cap, depth, d_tile)
    me = lax.axis_index("expert")
    z = me // PLANE
    q = me % PLANE
    y, x = q // 2, q % 2
    x_peer = y * 2 + (1 - x)
    y_peer = (1 - y) * 2 + x
    d_peer = (1 - y) * 2 + (1 - x)
    half = rows // 2

    weight_copies = [
        pltpu.make_async_copy(src.at[0], dst, w_sem.at[i])
        for i, (src, dst) in enumerate(((wg_hbm, wg), (wu_hbm, wu), (wd_hbm, wd)))
    ]
    own = pltpu.make_async_copy(tokens_hbm, gathered.at[me, :, pl.ds(0, depth)], own_sem)
    own.start()
    slot_rows = jnp.zeros((top, rows), jnp.int32)
    for e in range(table_ref.shape[1]):
        pair = jnp.where(choice_ref[...] == 0, table_ref[0, e], table_ref[1, e])
        slot_rows = jnp.where(ids_ref[...] == e, pair, slot_rows)
    folded[...] = jnp.zeros_like(folded)
    eye = (
        lax.broadcasted_iota(jnp.int32, (top, LANES), 0)
        == lax.broadcasted_iota(jnp.int32, (top, LANES), 1)
    ).astype(jnp.bfloat16)

    def turned(block):
        return lax.dot_general(
            block, eye, (((0,), (0,)), ((), ())), preferred_element_type=jnp.float32
        )

    slot_cols = turned(slot_rows.astype(jnp.float32).astype(jnp.bfloat16))
    k_lane = lax.broadcasted_iota(jnp.int32, (rows, LANES), 1)
    gathered[me, :, depth:] = jnp.where(k_lane < top, slot_cols, -1.0).astype(jnp.bfloat16)
    for copy in weight_copies:
        copy.start()

    barrier = pltpu.get_barrier_semaphore()
    for other in range(1, n):
        pl.semaphore_signal(
            barrier, inc=1, device_id={"expert": lax.rem(me + other, n)},
            device_id_type=pl.DeviceIdType.MESH,
        )
    pl.semaphore_wait(barrier, n - 1)
    own.wait()

    def send(group, plane, kind_send, kind_recv, target, first=0, count=None):
        count = rows if count is None else count
        part = gathered.at[group, pl.ds(first, count)]
        return pltpu.make_async_remote_copy(
            src_ref=part, dst_ref=part,
            send_sem=ag_send.at[plane, kind_send], recv_sem=ag_recv.at[plane, kind_recv],
            device_id={"expert": target}, device_id_type=pl.DeviceIdType.MESH,
        )

    z_half = planes // 2
    low = jnp.minimum(z, planes - 1 - z)

    def plane_at(b):
        pick = lax.rem(low + b, planes)
        return jnp.where(z < z_half, pick, planes - 1 - pick)

    order = [plane_at(b) for b in range(planes)]

    def across(p):
        return (p // z_half) != (z // z_half)

    def up_of(p):
        return send(p * PLANE + q, p, 0, 0, me + PLANE)

    def down_of(p):
        return send(p * PLANE + q, p, 1, 0, me - PLANE)

    def to_x(p):
        return send(p * PLANE + q, p, 2, 1, z * PLANE + x_peer)

    def to_y(p):
        return send(p * PLANE + q, p, 3, 2, z * PLANE + y_peer)

    def relay_y(p):
        return send(p * PLANE + x_peer, p, 4, 3, z * PLANE + y_peer, 0, half)

    def relay_x(p):
        return send(p * PLANE + y_peer, p, 5, 4, z * PLANE + x_peer, half, half)

    def wait_in(p, position, kind, first=0, count=None):
        count = rows if count is None else count
        part = gathered.at[p * PLANE + position, pl.ds(first, count)]
        pltpu.make_async_copy(part, part, ag_recv.at[p, kind]).wait()

    def column_stage(d):
        @pl.when(z - d >= 0)
        def _():
            wait_in(z - d, q, 0)

            @pl.when(z < planes - 1)
            def _():
                up_of(z - d).start()

        @pl.when(z + d < planes)
        def _():
            wait_in(z + d, q, 0)

            @pl.when(z > 0)
            def _():
                down_of(z + d).start()

    def spread_stage(p):
        to_x(p).start()
        to_y(p).start()

    def relay_stage(p):
        wait_in(p, x_peer, 1)
        relay_y(p).start()
        wait_in(p, y_peer, 2)
        relay_x(p).start()

    def diagonal_stage(p):
        wait_in(p, d_peer, 3, 0, half)
        wait_in(p, d_peer, 4, half, half)

    def return_copy(group):
        return pltpu.make_async_remote_copy(
            src_ref=outgoing.at[group], dst_ref=incoming.at[me],
            send_sem=ret_send.at[group], recv_sem=ret_recv.at[me],
            device_id={"expert": group}, device_id_type=pl.DeviceIdType.MESH,
        )

    def own_return():
        return pltpu.make_async_copy(outgoing.at[me], incoming.at[me], local_sem)

    batch_tokens = PLANE * rows
    batch_rows = PLANE * pad
    t_i = lax.broadcasted_iota(jnp.int32, (batch_tokens, batch_tokens), 0)
    t_j = lax.broadcasted_iota(jnp.int32, (batch_tokens, batch_tokens), 1)
    before = ((t_j < t_i) & (t_j // rows == t_i // rows)).astype(jnp.bfloat16)
    lane = lax.broadcasted_iota(jnp.int32, (batch_tokens, batch_rows), 1).astype(jnp.float32)
    base = (
        lax.broadcasted_iota(jnp.int32, (batch_tokens, batch_rows), 0) // rows * pad
    ).astype(jnp.float32)
    me_f = me.astype(jnp.float32)
    ff_tile = tile_of(hidden, 256)

    def compute(p, first):
        ids = gathered[pl.ds(p * PLANE, PLANE), :, depth:].reshape(batch_tokens, LANES)
        hit = jnp.sum((ids.astype(jnp.float32) == me_f).astype(jnp.float32), axis=1, keepdims=True)
        pos = jnp.dot(
            before, jnp.broadcast_to(hit, (batch_tokens, batch_rows)).astype(jnp.bfloat16),
            preferred_element_type=jnp.float32,
        )
        kept = (hit > 0.5) & (pos < cap - 0.5)
        chosen = (kept & (lane == base + pos)).astype(jnp.float32)
        chosen_count = chosen
        chosen = chosen.astype(jnp.bfloat16)

        @pl.loop(0, depth // d_tile, unroll=2)
        def _(i):
            cols = pl.ds(pl.multiple_of(i * d_tile, d_tile), d_tile)
            block = gathered[pl.ds(p * PLANE, PLANE), :, cols].reshape(batch_tokens, d_tile)
            packed[:, cols] = lax.dot_general(
                chosen, block, (((0,), (0,)), ((), ())), preferred_element_type=jnp.float32
            ).astype(jnp.bfloat16)

        if first:
            weight_copies[0].wait()
            weight_copies[1].wait()

        @pl.loop(0, hidden // ff_tile)
        def _(i):
            cols = pl.ds(pl.multiple_of(i * ff_tile, ff_tile), ff_tile)
            gate = jnp.dot(packed[...], wg[:, cols], preferred_element_type=jnp.float32)
            up = jnp.dot(packed[...], wu[:, cols], preferred_element_type=jnp.float32)
            mid[:, cols] = (gate / (1.0 + jnp.exp(-gate)) * up).astype(jnp.bfloat16)

        if first:
            weight_copies[2].wait()

        @pl.loop(0, depth // d_tile, unroll=2)
        def _(i):
            cols = pl.ds(pl.multiple_of(i * d_tile, d_tile), d_tile)
            out = jnp.dot(mid[...], wd[:, cols], preferred_element_type=jnp.float32)
            out = out.reshape(PLANE, pad, d_tile)
            for slab in range(full):
                at = pl.ds(pl.multiple_of(slab * depth + i * d_tile, d_tile), d_tile)
                outgoing[pl.ds(p * PLANE, PLANE), :, at] = out[
                    :, slab * 8 : slab * 8 + 8
                ].astype(jnp.bfloat16)
            for start, count, _, width, offset in pieces:
                steps = width // d_tile
                at = pl.ds(
                    pl.multiple_of(offset - full * depth + i % steps * d_tile, d_tile), d_tile
                )
                for r in range(count):
                    folded[:, pl.ds(i // steps * count + r, 1), at] = out[
                        :, start + r : start + r + 1
                    ]

        if pieces:
            outgoing[pl.ds(p * PLANE, PLANE), :, full * depth :] = folded[...].astype(
                jnp.bfloat16
            )
        return jnp.sum(chosen_count)

    def give_back(p):
        for j in range(PLANE):
            group = p * PLANE + j

            @pl.when(group != me)
            def _():
                return_copy(group).start()

            @pl.when(group == me)
            def _():
                own_return().start()

    accepted = jnp.float32(0.0)

    @pl.when(z < planes - 1)
    def _():
        up_of(z).start()

    @pl.when(z > 0)
    def _():
        down_of(z).start()

    spread_stage(order[0])
    column_stage(1)
    spread_stage(order[1])
    relay_stage(order[0])
    column_stage(2)
    relay_stage(order[1])
    spread_stage(order[2])
    turns = [1, 0] + list(range(2, planes))
    for i, b in enumerate(turns):
        diagonal_stage(order[b])
        accepted += compute(order[b], i == 0)

        @pl.when(across(order[b]))
        def _():
            give_back(order[b])

        if i + 3 < planes:
            column_stage(i + 3)
            relay_stage(order[i + 2])
            spread_stage(order[i + 3])
        elif i + 2 < planes:
            relay_stage(order[i + 2])

    for b in turns:

        @pl.when(jnp.logical_not(across(order[b])))
        def _():
            give_back(order[b])

    load_ref[0] = accepted * (n / (rows * n * top))

    g_high = gates_ref[...].astype(jnp.bfloat16)
    g_rest = gates_ref[...] - g_high.astype(jnp.float32)
    g_middle = g_rest.astype(jnp.bfloat16)
    g_low = (g_rest - g_middle.astype(jnp.float32)).astype(jnp.bfloat16)
    gate_cols = turned(g_high) + (turned(g_middle) + turned(g_low))
    own_lane = lax.broadcasted_iota(jnp.int32, (rows, LANES), 1).astype(jnp.float32)
    slots = [slot_cols[:, k : k + 1] for k in range(top)]
    hits = functools.reduce(jnp.add, [(s == own_lane).astype(jnp.float32) for s in slots])
    r_i = lax.broadcasted_iota(jnp.int32, (rows, rows), 0)
    r_j = lax.broadcasted_iota(jnp.int32, (rows, rows), 1)
    positions = jnp.dot(
        (r_j < r_i).astype(jnp.bfloat16), hits.astype(jnp.bfloat16),
        preferred_element_type=jnp.float32,
    )
    columns, weights, inside_plane = [], [], []
    for k in range(top):
        at = jnp.sum(jnp.where(slots[k] == own_lane, positions, 0.0), axis=1, keepdims=True)
        lane_of = at + (PLANE * 8 - 8) * jnp.floor(at * 0.125)
        moves = []
        for index, (start, count, _, _, _) in enumerate(pieces):
            inside = (at > start - 0.5) & (at < start + count - 0.5)
            lane_of = jnp.where(inside, (full + index) * PLANE * 8 + at - start, lane_of)
            moves.append(jnp.where(inside, float(count), 0.0))
        columns.append((slots[k] * 8 + lane_of, moves))
        weights.append(jnp.where(at < cap - 0.5, gate_cols[:, k : k + 1], 0.0))
        inside_plane.append(jnp.floor(slots[k] * (1.0 / PLANE)))
    stacked = (full + len(pieces)) * PLANE * 8
    col_lane = lax.broadcasted_iota(jnp.int32, (rows, stacked), 1).astype(jnp.float32)

    @pl.loop(0, planes)
    def _(p):
        p_f = p.astype(jnp.float32)
        here = [jnp.where(g == p_f, w, 0.0) for g, w in zip(inside_plane, weights)]

        @pl.loop(0, depth // d_tile)
        def _(i):
            shifts = [
                (i // (width // d_tile)).astype(jnp.float32) for _, _, _, width, _ in pieces
            ]
            share = jnp.zeros((rows, stacked), jnp.float32)
            for (lane_of, moves), w in zip(columns, here):
                at = lane_of - p_f * (PLANE * 8)
                for move, shift in zip(moves, shifts):
                    at = at + move * shift
                share = share + jnp.where(at == col_lane, w, 0.0)
            high = share.astype(jnp.bfloat16)
            rest = share - high.astype(jnp.float32)
            middle = rest.astype(jnp.bfloat16)
            low = (rest - middle.astype(jnp.float32)).astype(jnp.bfloat16)
            spreads[p, i] = jnp.concatenate([high, middle, low], axis=0)

    for step in range(planes):
        turn = lax.rem(z // z_half + 1 + step // z_half, 2)
        turn = 1 - turn
        inner = step % z_half
        p = turn * z_half + jnp.where(turn == 0, z_half - 1 - inner, inner)
        for j in range(PLANE):
            source = p * PLANE + j

            @pl.when(source != me)
            def _():
                block = incoming.at[source]
                pltpu.make_async_copy(block, block, ret_recv.at[source]).wait()

            @pl.when(source == me)
            def _():
                own_return().wait()


        @pl.loop(0, depth // d_tile, unroll=2)
        def _(i):
            cols = pl.ds(pl.multiple_of(i * d_tile, d_tile), d_tile)
            offsets = [slab * depth + i * d_tile for slab in range(full)]
            for _, _, _, width, offset in pieces:
                offsets.append(offset + i % (width // d_tile) * d_tile)
            spread = spreads[p, i]
            slabs = [
                incoming[
                    pl.ds(p * PLANE, PLANE), :, pl.ds(pl.multiple_of(o, d_tile), d_tile)
                ].astype(jnp.float32).reshape(PLANE * 8, d_tile)
                for o in offsets
            ]
            block = jnp.concatenate(slabs, axis=0).astype(jnp.bfloat16)
            sums = jnp.dot(spread, block, preferred_element_type=jnp.float32)
            sums = sums[:rows] + (sums[rows : 2 * rows] + sums[2 * rows :])
            if step > 0:
                sums = acc[:, cols] + sums
            if step < planes - 1:
                acc[:, cols] = sums
            else:
                mixed_ref[:, cols] = sums.astype(jnp.bfloat16)

    for b in range(planes):
        p = order[b]

        @pl.when((p <= z) & (z < planes - 1))
        def _():
            up_of(p).wait_send()

        @pl.when((p >= z) & (z > 0))
        def _():
            down_of(p).wait_send()

        to_x(p).wait_send()
        to_y(p).wait_send()
        relay_y(p).wait_send()
        relay_x(p).wait_send()
        for j in range(PLANE):
            group = p * PLANE + j

            @pl.when(group != me)
            def _():
                return_copy(group).wait_send()


def per_device_gathered(
    tokens, expert_ids, gate_weights, placement_table, replica_choice, w_gate, w_up, w_down
):
    n = lax.axis_size("expert")
    rows, top = expert_ids.shape
    depth = tokens.shape[1]
    hidden = w_gate.shape[2]
    cap = 5 * rows * top // (4 * n) + 1
    slabs = -(-cap // 8)
    d_tile = tile_of(depth, D_TILE)
    full, pieces, length = folds_of(cap, depth, d_tile)
    stacked = (full + len(pieces)) * PLANE * 8
    planes = n // PLANE
    bf16, f32 = jnp.bfloat16, jnp.float32
    anywhere = pl.BlockSpec(memory_space=pl.ANY)
    vmem = pl.BlockSpec(memory_space=pltpu.VMEM)
    smem = pl.BlockSpec(memory_space=pltpu.SMEM)
    mixed, load = pl.pallas_call(
        functools.partial(kernel, n, rows, top, cap, depth, hidden),
        out_shape=(
            jax.ShapeDtypeStruct((rows, depth), bf16),
            jax.ShapeDtypeStruct((1,), f32),
        ),
        in_specs=[smem, anywhere, vmem, vmem, vmem, anywhere, anywhere, anywhere],
        out_specs=(vmem, smem),
        scratch_shapes=[
            pltpu.VMEM((n, rows, depth + LANES), bf16),
            pltpu.VMEM((depth, hidden), bf16),
            pltpu.VMEM((depth, hidden), bf16),
            pltpu.VMEM((hidden, depth), bf16),
            pltpu.VMEM((PLANE * slabs * 8, depth), bf16),
            pltpu.VMEM((PLANE * slabs * 8, hidden), bf16),
            pltpu.VMEM((n, 8, length), bf16),
            pltpu.VMEM((n, 8, length), bf16),
            pltpu.VMEM((rows, depth), f32),
            pltpu.VMEM((PLANE, 8, max(length - cap // 8 * depth, LANES)), f32),
            pltpu.VMEM((planes, depth // d_tile, 3 * rows, stacked), bf16),
            pltpu.SemaphoreType.DMA((3,)),
            pltpu.SemaphoreType.DMA,
            pltpu.SemaphoreType.DMA((planes, 6)),
            pltpu.SemaphoreType.DMA((planes, 5)),
            pltpu.SemaphoreType.DMA((n,)),
            pltpu.SemaphoreType.DMA((n,)),
            pltpu.SemaphoreType.DMA,
        ],
        compiler_params=pltpu.CompilerParams(
            collective_id=0, has_side_effects=True, vmem_limit_bytes=VMEM_BYTES
        ),
    )(
        placement_table.T, tokens, expert_ids.T, replica_choice.T, gate_weights.T,
        w_gate, w_up, w_down,
    )
    return mixed, load


def solution(mesh):
    placed = (
        P(("dp", "expert"), None),
        P(("dp", "expert"), None),
        P(("dp", "expert"), None),
        P("dp", None),
        P(("dp", "expert"), None),
        P("expert", None, None),
        P("expert", None, None),
        P("expert", None, None),
    )

    def per_device(*args):
        n = mesh.shape["expert"]
        rows, depth = args[0].shape
        weights = 3 * args[5].size
        blocks = n * rows * (depth + LANES) + 2 * n * (rows + 8) * depth
        fits = 2 * (weights + blocks) < 3 * VMEM_BYTES // 4
        if fits and n % (2 * PLANE) == 0 and n > 2 * PLANE and n <= LANES and rows % 16 == 0:
            return per_device_gathered(*args)
        return per_device_exchange(*args)

    return jax.shard_map(
        per_device,
        mesh=mesh,
        in_specs=placed,
        out_specs=(P(("dp", "expert"), None), P(("dp", "expert"))),
        check_vma=False,
    )
```
